32 devices in a mesh: subj: 4 (over y, x), cortex: 8 (over z, core).
Axes of the slice: x: 2, y: 2, z: 4, core: 2. Of those that a mesh axis runs over, the one named last changes fastest.
Arguments:
- series: bfloat16 [8, 1024, 2048], P('subj', None, 'cortex'), may hold values from -6 to 6
- template: bfloat16 [1024, 2048], P(None, 'cortex'), may hold values from -6 to 6
- sl_blocks: int32 [16, 3], P('cortex'), may hold values from 0 to 15, as said below
Outputs:
- template_new: float32 [1024, 2048], P(None, 'cortex')
The draws below stay inside these ranges and needn't reach their ends.
Inputs may be any that keep to these rules, and one draw needn't show every extreme that they name: sl_blocks[g, 0] = g; the other two entries of row g are distinct, differ from g, and lie between (g // 2 - 1) * 2 and (g // 2 + 2) * 2 - 1.
All inputs are finite; a program needn't handle non-finite values.
Results may differ from the reference program's by a relative error of at most 0.0024.
Values may be sent and summed in bfloat16 or wider, within the bound.
No kernel may reach another device: no remote copies, remote signals or barrier semaphores. Data moves between devices by JAX's collectives and lax.ppermute only.
A program may use at most 64 MiB of HBM per device.

```python
import jax
import jax.numpy as jnp
from jax import lax

BLOCK = 128
NS_STEPS = 8
FRAMES = 1024
BLK_DEV = 2
SUBJECTS = 8
NBLOCKS = 16
VERTS = 2048


def draw_sl_blocks(key, part):
    first_key, second_key = jax.random.split(jax.random.fold_in(key, 7))
    centre = jnp.arange(NBLOCKS, dtype=jnp.int32)
    owner_dev = centre // BLK_DEV
    window_low = jnp.maximum((owner_dev - 1) * BLK_DEV, 0)
    window_high = jnp.minimum((owner_dev + 2) * BLK_DEV, NBLOCKS)
    span_size = window_high - window_low
    position = centre - window_low
    first_pick = jax.random.randint(first_key, (NBLOCKS,), 0, span_size - 1)
    first_pick = first_pick + (first_pick >= position).astype(jnp.int32)
    lower_mark = jnp.minimum(position, first_pick)
    upper_mark = jnp.maximum(position, first_pick)
    second_pick = jax.random.randint(second_key, (NBLOCKS,), 0, span_size - 2)
    second_pick = second_pick + (second_pick >= lower_mark).astype(jnp.int32)
    second_pick = second_pick + (second_pick >= upper_mark).astype(jnp.int32)
    return jnp.stack([centre, window_low + first_pick, window_low + second_pick], axis=1).astype(jnp.int32)


def shard_levels(key, dims, cuts, least, largest):
    def one(dim, parts):
        draws = jax.random.uniform(jax.random.fold_in(jax.random.fold_in(key, 6), dim), (parts,), jnp.float32, least / len(cuts), largest / len(cuts))
        return jnp.repeat(jnp.exp(draws), dims[dim] // parts).reshape((-1,) + (1,) * (len(dims) - dim - 1))

    gain = one(*cuts[0])
    for cut in cuts[1:]:
        gain = gain * one(*cut)
    return gain


def bell_draw(key, extent, spread, bound, cuts=(), kind=jnp.bfloat16):
    result = jax.random.normal(key, extent, jnp.float32) * spread
    if len(cuts) > 0:
        result = shard_levels(key, extent, cuts, -0.22, 0.18) * result
    return jnp.clip(result, min=-bound, max=bound).astype(kind)


def setup_inputs(seed: int = 0) -> dict:
    key_list = jax.random.split(jax.random.key(seed), 4)
    series = bell_draw(key_list[0], (SUBJECTS, FRAMES, VERTS), 1.0, 6.0, ((0, 4), (2, 8)))
    template = bell_draw(key_list[1], (FRAMES, VERTS), 1.0, 6.0, ((1, 8),))
    sl_blocks = draw_sl_blocks(jax.random.fold_in(key_list[3], 71), 0)
    return {"series": series, "template": template, "sl_blocks": sl_blocks}


RIDGE_SHIFT = 0.1
NORM_EPSILON = 1e-06

def rounded(value):
    return lax.optimization_barrier(value.astype(jnp.bfloat16))

def polar_factor(cross_prod):
    squares = lax.optimization_barrier(jnp.sum(cross_prod * cross_prod, axis=(1, 2), keepdims=True))
    current = rounded(cross_prod / jnp.sqrt(squares + NORM_EPSILON))
    for iteration in range(NS_STEPS):
        wide_map = current.astype(jnp.float32)
        gram_mat = rounded(jnp.einsum('sab,sac->sbc', wide_map, wide_map, precision=lax.Precision.HIGHEST))
        product = jnp.einsum('sab,sbc->sac', wide_map, gram_mat.astype(jnp.float32), precision=lax.Precision.HIGHEST)
        current = rounded(1.5 * wide_map - 0.5 * product)
    return current

def reference(series, template, sl_blocks):
    subj_count = series.shape[0]
    offsets = jnp.arange(BLOCK, dtype=jnp.int32)
    identity = jnp.eye(3 * BLOCK, dtype=jnp.float32)

    def visit_one(running, blocks):
        columns = (blocks[:, None] * BLOCK + offsets[None, :]).reshape(-1).astype(jnp.int32)
        subj_cols = jnp.take(series, columns, axis=2).astype(jnp.float32)
        tmpl_cols = jnp.take(template, columns, axis=1).astype(jnp.float32)
        cross_prod = jnp.einsum('sfa,fb->sab', subj_cols, tmpl_cols, precision=lax.Precision.HIGHEST) / FRAMES + RIDGE_SHIFT * identity
        polar_map = polar_factor(cross_prod)
        mapped = jnp.einsum('sfa,sab->sfb', subj_cols, polar_map.astype(jnp.float32), precision=lax.Precision.HIGHEST)
        running = running.at[:, columns].add(lax.optimization_barrier(jnp.sum(mapped, axis=0)))
        return (running, None)
    running = jnp.zeros((FRAMES, VERTS), jnp.float32)
    running, unused = lax.scan(visit_one, running, sl_blocks)
    block_ids = sl_blocks.reshape(-1)
    coverage = lax.optimization_barrier(jnp.sum((block_ids[:, None] == jnp.arange(NBLOCKS, dtype=jnp.int32)[None, :]).astype(jnp.float32), axis=0))
    per_vertex = jnp.repeat(coverage, BLOCK)
    return running / per_vertex[None, :] / subj_count
```

```python
import functools

import jax
import jax.numpy as jnp
from jax import lax
from jax.experimental import pallas as pl
from jax.experimental.pallas import tpu as pltpu
from jax.sharding import PartitionSpec as P

BLOCK = 128
NS_STEPS = 8
RIDGE_SHIFT = 0.1
NORM_EPSILON = 1e-06
MIB = 1 << 20


def swap_near(value):
    count = lax.axis_size("cortex")
    return lax.ppermute(value, "cortex", [(i, i ^ 1) for i in range(count)])


def swap_far(value):
    count = lax.axis_size("cortex")
    route = [(0, 0), (count - 1, count - 1)]
    for i in range(1, count - 1, 2):
        route += [(i, i + 1), (i + 1, i)]
    return lax.ppermute(value, "cortex", route)


def swap_subj(value, distance):
    count = lax.axis_size("subj")
    return lax.ppermute(value, "subj", [(i, i ^ distance) for i in range(count)])


def vmem():
    return pl.BlockSpec(memory_space=pltpu.VMEM)


def smem():
    return pl.BlockSpec(memory_space=pltpu.SMEM)


def call(kernel, out_shape, in_specs, flops, limit, scratch=(), name=None):
    outs = jax.tree.leaves(out_shape)
    return pl.pallas_call(
        kernel,
        out_shape=out_shape,
        in_specs=in_specs,
        out_specs=jax.tree.map(lambda _: vmem(), out_shape),
        scratch_shapes=list(scratch),
        compiler_params=pltpu.CompilerParams(vmem_limit_bytes=limit * MIB),
        cost_estimate=pl.CostEstimate(
            flops=flops, bytes_accessed=sum(o.size * o.dtype.itemsize for o in outs), transcendentals=0
        ),
        name=name,
    )


def columns(ref, half):
    return ref[:, pl.ds(pl.multiple_of(half * BLOCK, BLOCK), BLOCK)]


def template_kernel(code_ref, own_ref, near_ref, far_ref, out_ref):
    lights, members = code_ref.shape
    for g in range(lights):
        for j in range(members):
            code = code_ref[g, j]
            for place, ref in enumerate((own_ref, near_ref, far_ref)):

                @pl.when(code // 2 == place)
                def _():
                    out_ref[g, j * BLOCK : (j + 1) * BLOCK, :] = columns(ref, code % 2).T


def polar_kernel(code_ref, tmpl_ref, own_ref, near_ref, far_ref, map_ref, cols_ref):
    lights, members = code_ref.shape
    width = members * BLOCK
    frames = own_ref.shape[0]
    for g in range(lights):
        for i in range(members):
            code = code_ref[g, i]
            lo = g * width + i * BLOCK
            for place, ref in enumerate((own_ref, near_ref, far_ref)):

                @pl.when(code // 2 == place)
                def _():
                    cols_ref[:, lo : lo + BLOCK] = columns(ref, code % 2)

    row = lax.broadcasted_iota(jnp.int32, (width, width), 0)
    col = lax.broadcasted_iota(jnp.int32, (width, width), 1)
    ridge = jnp.where(row == col, RIDGE_SHIFT, 0.0)
    for g in range(lights):
        cross = jnp.dot(
            tmpl_ref[g], cols_ref[:, g * width : (g + 1) * width], preferred_element_type=jnp.float32
        )
        cross = cross * (1.0 / frames) + ridge
        squares = jnp.sum(cross * cross, keepdims=True)
        map_ref[g] = (cross * (1.0 / jnp.sqrt(squares + NORM_EPSILON))).astype(jnp.bfloat16)

    def step(_, carry):
        for g in range(lights):
            now = map_ref[g]
            gram = lax.dot_general(
                now, now, (((1,), (1,)), ((), ())), preferred_element_type=jnp.float32
            ).astype(jnp.bfloat16)
            product = jnp.dot(gram, now, preferred_element_type=jnp.float32)
            map_ref[g] = (1.5 * now.astype(jnp.float32) - 0.5 * product).astype(jnp.bfloat16)
        return carry

    lax.fori_loop(0, NS_STEPS, step, 0)


def map_kernel(subj_count, places, code_ref, *refs):
    cols_refs = refs[:subj_count]
    map_refs = refs[subj_count : 2 * subj_count]
    weight_ref = refs[-1]
    out_refs = refs[2 * subj_count : -1]
    lights, members = code_ref.shape
    width = members * BLOCK
    for p, place in enumerate(places):
        for g in range(lights):
            pick = jnp.int32(0)
            found = code_ref[g, 0] == place
            for j in range(1, members):
                hit = code_ref[g, j] == place
                pick = jnp.where(hit, j, pick)
                found = jnp.logical_or(found, hit)
            rows = pl.ds(pl.multiple_of(pick * BLOCK, BLOCK), BLOCK)
            for s in range(subj_count):
                lo = (s * lights + g) * width
                piece = map_refs[s][g, rows, :]
                weight_ref[p * BLOCK : (p + 1) * BLOCK, lo : lo + width] = jnp.where(
                    found, piece, jnp.zeros_like(piece)
                )
    depth = lights * width
    chunk = 256
    start = 0
    step_cols = 2 * BLOCK
    for first in range(0, len(places) * BLOCK, step_cols):
        weights = [
            weight_ref[first : first + step_cols, s * depth : (s + 1) * depth] for s in range(subj_count)
        ]
        group = out_refs[start]
        start += 1
        for lo in range(0, cols_refs[0].shape[0], chunk):
            total = None
            for s in range(subj_count):
                term = lax.dot_general(
                    cols_refs[s][lo : lo + chunk, :],
                    weights[s],
                    (((1,), (1,)), ((), ())),
                    preferred_element_type=jnp.float32,
                )
                total = term if total is None else total + term
            group[lo : lo + chunk, :] = total.astype(group.dtype)


def body(series, template, sl_blocks):
    subj_count, frames, width_dev = series.shape
    lights, members = sl_blocks.shape
    blk_dev = width_dev // BLOCK
    width = members * BLOCK
    count = lax.axis_size("cortex")
    position = lax.axis_index("cortex")
    odd = position % 2
    far_real = jnp.logical_and(position + 2 * odd - 1 >= 0, position + 2 * odd - 1 < count)

    tmpl_far = swap_far(template)
    tmpl_near = swap_near(template)
    parts = [series[s] for s in range(subj_count)]
    far = [swap_far(p) for p in parts]
    near = [swap_near(p) for p in parts]
    lists_near = swap_near(sl_blocks)
    lists_far = swap_far(sl_blocks)

    window = sl_blocks - (position - 1) * blk_dev
    side = window // blk_dev
    place = jnp.where(side == 1, 0, jnp.where((side == 2) == (odd == 1), 2, 1))
    code = (place * blk_dev + window % blk_dev).astype(jnp.int32)

    mine = position * blk_dev + jnp.arange(blk_dev, dtype=jnp.int32)

    def counted(lists):
        return jnp.sum((lists.reshape(-1)[:, None] == mine[None, :]).astype(jnp.float32), axis=0)

    coverage = counted(sl_blocks) + counted(lists_near) + jnp.where(far_real, counted(lists_far), 0.0)
    per_vertex = jnp.repeat(coverage, BLOCK)

    tmpl_rows = call(
        template_kernel,
        jax.ShapeDtypeStruct((lights, width, frames), jnp.bfloat16),
        [smem(), vmem(), vmem(), vmem()],
        flops=10**9,
        limit=16,
        name="template_rows",
    )(code, template, tmpl_near, tmpl_far)

    maps, cols = [], []
    for s in range(subj_count):
        polar, gathered = call(
            polar_kernel,
            (
                jax.ShapeDtypeStruct((lights, width, width), jnp.bfloat16),
                jax.ShapeDtypeStruct((frames, lights * width), jnp.bfloat16),
            ),
            [smem()] + [vmem()] * 4,
            flops=8 * 10**9,
            limit=24,
            name="polar",
        )(code, tmpl_rows, parts[s], near[s], far[s])
        maps.append(polar)
        cols.append(gathered)

    def mapped(places, types, name):
        shapes = [jax.ShapeDtypeStruct((frames, 2 * BLOCK), t) for t in types]
        return call(
            functools.partial(map_kernel, subj_count, places),
            shapes,
            [smem()] + [vmem()] * (2 * subj_count),
            flops=2 * 10**9,
            limit=24,
            scratch=[pltpu.VMEM((len(places) * BLOCK, subj_count * lights * width), jnp.bfloat16)],
            name=name,
        )(code, *cols, *maps)

    (to_far,) = mapped((4, 5), (jnp.bfloat16,), "map_far")
    from_far = swap_far(to_far)
    to_near, own = mapped((2, 3, 0, 1), (jnp.bfloat16, jnp.float32), "map_rest")
    from_near = swap_near(to_near)
    keep = far_real.astype(jnp.float32)
    own_sum = own + from_near.astype(jnp.float32) + keep * from_far.astype(jnp.float32)

    subj_size = lax.axis_size("subj")
    distances = []
    while 2 ** len(distances) < subj_size:
        distances.append(2 ** len(distances))
    rows = frames // 2
    halves = [own_sum[:rows], own_sum[rows:]]
    for step in range(len(distances)):
        for h in range(2):
            sent = halves[h].astype(jnp.bfloat16)
            got = swap_subj(sent, distances[(step + h) % len(distances)])
            halves[h] = sent.astype(jnp.float32) + got.astype(jnp.float32)
    total = jnp.concatenate(halves, axis=0)
    return total / per_vertex[None, :] / (subj_count * subj_size)


def solution(mesh):
    in_specs = (P("subj", None, "cortex"), P(None, "cortex"), P("cortex", None))
    out_specs = P(None, "cortex")
    return jax.shard_map(body, mesh=mesh, in_specs=in_specs, out_specs=out_specs, check_vma=False)
```

```python
import functools

import jax
import jax.numpy as jnp
from jax import lax
from jax.experimental import pallas as pl
from jax.experimental.pallas import tpu as pltpu
from jax.sharding import PartitionSpec as P


BLOCK = 128
NS_STEPS = 8
RIDGE_SHIFT = 0.1
NORM_EPSILON = 1e-06
MIB = 1 << 20


def swap_near(value):
    count = lax.axis_size("cortex")
    return lax.ppermute(value, "cortex", [(i, i ^ 1) for i in range(count)])


def swap_far(value):
    count = lax.axis_size("cortex")
    route = [(0, 0), (count - 1, count - 1)]
    for i in range(1, count - 1, 2):
        route += [(i, i + 1), (i + 1, i)]
    return lax.ppermute(value, "cortex", route)


def swap_subj(value, distance):
    count = lax.axis_size("subj")
    return lax.ppermute(value, "subj", [(i, i ^ distance) for i in range(count)])


def vmem():
    return pl.BlockSpec(memory_space=pltpu.VMEM)


def smem():
    return pl.BlockSpec(memory_space=pltpu.SMEM)


def call(kernel, out_shape, in_specs, flops, limit, scratch=()):
    outs = jax.tree.leaves(out_shape)
    return pl.pallas_call(
        kernel,
        out_shape=out_shape,
        in_specs=in_specs,
        out_specs=jax.tree.map(lambda _: vmem(), out_shape),
        scratch_shapes=list(scratch),
        compiler_params=pltpu.CompilerParams(vmem_limit_bytes=limit * MIB),
        cost_estimate=pl.CostEstimate(
            flops=flops, bytes_accessed=sum(o.size * o.dtype.itemsize for o in outs), transcendentals=0
        ),
    )


def columns(ref, half):
    return ref[:, pl.ds(pl.multiple_of(half * BLOCK, BLOCK), BLOCK)]


def template_kernel(code_ref, own_ref, near_ref, far_ref, out_ref):
    lights, members = code_ref.shape
    for g in range(lights):
        for j in range(members):
            code = code_ref[g, j]
            for place, ref in enumerate((own_ref, near_ref, far_ref)):

                @pl.when(code // 2 == place)
                def _():
                    out_ref[g, j * BLOCK : (j + 1) * BLOCK, :] = columns(ref, code % 2).T


def newton_schulz(now):
    head = now.shape[0] - BLOCK
    top, low = now[:head], now[head:]
    over = (((1,), (1,)), ((), ()))
    corner = lax.dot_general(top, top, over, preferred_element_type=jnp.float32).astype(jnp.bfloat16)
    bottom = lax.dot_general(low, now, over, preferred_element_type=jnp.float32).astype(jnp.bfloat16)
    gram = jnp.concatenate([jnp.concatenate([corner, bottom[:, :head].T], axis=1), bottom], axis=0)
    product = jnp.dot(gram, now, preferred_element_type=jnp.float32)
    return (1.5 * now.astype(jnp.float32) - 0.5 * product).astype(jnp.bfloat16)


def polar_kernel(code_ref, tmpl_ref, own_ref, near_ref, far_ref, map_ref, cols_ref):
    lights, members = code_ref.shape
    width = members * BLOCK
    frames = own_ref.shape[0]
    for g in range(lights):
        for i in range(members):
            code = code_ref[g, i]
            lo = g * width + i * BLOCK
            for place, ref in enumerate((own_ref, near_ref, far_ref)):

                @pl.when(code // 2 == place)
                def _():
                    cols_ref[:, lo : lo + BLOCK] = columns(ref, code % 2)

    row = lax.broadcasted_iota(jnp.int32, (width, width), 0)
    col = lax.broadcasted_iota(jnp.int32, (width, width), 1)
    ridge = jnp.where(row == col, RIDGE_SHIFT, 0.0)
    for g in range(lights):
        cross = jnp.dot(
            tmpl_ref[g], cols_ref[:, g * width : (g + 1) * width], preferred_element_type=jnp.float32
        )
        cross = cross * (1.0 / frames) + ridge
        squares = jnp.sum(cross * cross, keepdims=True)
        map_ref[g] = (cross * (1.0 / jnp.sqrt(squares + NORM_EPSILON))).astype(jnp.bfloat16)

    for _ in range(NS_STEPS):
        for g in range(lights):
            map_ref[g] = newton_schulz(map_ref[g])


def map_kernel(subj_count, places, splits, code_ref, *refs):
    cols_refs = refs[:subj_count]
    map_refs = refs[subj_count : 2 * subj_count]
    weight_ref = refs[-1]
    out_refs = refs[2 * subj_count : -1]
    lights, members = code_ref.shape
    width = members * BLOCK
    for p, place in enumerate(places):
        for g in range(lights):
            pick = jnp.int32(0)
            found = code_ref[g, 0] == place
            for j in range(1, members):
                hit = code_ref[g, j] == place
                pick = jnp.where(hit, j, pick)
                found = jnp.logical_or(found, hit)
            rows = pl.ds(pl.multiple_of(pick * BLOCK, BLOCK), BLOCK)
            for s in range(subj_count):
                lo = (s * lights + g) * width
                piece = map_refs[s][g, rows, :]
                weight_ref[p * BLOCK : (p + 1) * BLOCK, lo : lo + width] = jnp.where(
                    found, piece, jnp.zeros_like(piece)
                )
    depth = lights * width
    step_cols = len(places) * BLOCK // len(splits)
    chunk = 256
    at = 0
    for n, pieces in enumerate(splits):
        first = n * step_cols
        weights = [
            weight_ref[first : first + step_cols, s * depth : (s + 1) * depth] for s in range(subj_count)
        ]
        rows = cols_refs[0].shape[0] // pieces
        for piece in range(pieces):
            for lo in range(0, rows, chunk):
                total = None
                for s in range(subj_count):
                    term = lax.dot_general(
                        cols_refs[s][piece * rows + lo : piece * rows + lo + chunk, :],
                        weights[s],
                        (((1,), (1,)), ((), ())),
                        preferred_element_type=jnp.float32,
                    )
                    total = term if total is None else total + term
                out_refs[at][lo : lo + chunk, :] = total.astype(out_refs[at].dtype)
            at += 1


def body(series, template, sl_blocks):
    subj_count, frames, width_dev = series.shape
    lights, members = sl_blocks.shape
    blk_dev = width_dev // BLOCK
    width = members * BLOCK
    count = lax.axis_size("cortex")
    position = lax.axis_index("cortex")
    odd = position % 2
    far_real = jnp.logical_and(position + 2 * odd - 1 >= 0, position + 2 * odd - 1 < count)

    tmpl_far = swap_far(template)
    tmpl_near = swap_near(template)
    parts = [series[s] for s in range(subj_count)]
    far, near = [], []
    for part in parts:
        far.append(swap_far(part))
        near.append(swap_near(part))
    lists_near = swap_near(sl_blocks)
    lists_far = swap_far(sl_blocks)

    window = sl_blocks - (position - 1) * blk_dev
    side = window // blk_dev
    place = jnp.where(side == 1, 0, jnp.where((side == 2) == (odd == 1), 2, 1))
    code = (place * blk_dev + window % blk_dev).astype(jnp.int32)

    mine = position * blk_dev + jnp.arange(blk_dev, dtype=jnp.int32)

    def counted(lists):
        return jnp.sum((lists.reshape(-1)[:, None] == mine[None, :]).astype(jnp.float32), axis=0)

    coverage = counted(sl_blocks) + counted(lists_near) + jnp.where(far_real, counted(lists_far), 0.0)
    per_vertex = jnp.repeat(coverage, BLOCK)

    tmpl_rows = call(
        template_kernel,
        jax.ShapeDtypeStruct((lights, width, frames), jnp.bfloat16),
        [smem(), vmem(), vmem(), vmem()],
        flops=10**9,
        limit=16,
    )(code, template, tmpl_near, tmpl_far)

    maps, cols = [], []
    for s in range(subj_count):
        if s == subj_count - 1:
            code, per_vertex = lax.optimization_barrier((code, per_vertex))
        polar, gathered = call(
            polar_kernel,
            (
                jax.ShapeDtypeStruct((lights, width, width), jnp.bfloat16),
                jax.ShapeDtypeStruct((frames, lights * width), jnp.bfloat16),
            ),
            [smem()] + [vmem()] * 4,
            flops=8 * 10**9,
            limit=24,
        )(code, tmpl_rows, parts[s], near[s], far[s])
        maps.append(polar)
        cols.append(gathered)

    def mapped(code, places, splits, types):
        shapes = [
            jax.ShapeDtypeStruct((frames // pieces, width_dev), kind)
            for pieces, kind in zip(splits, types)
            for _ in range(pieces)
        ]
        return call(
            functools.partial(map_kernel, subj_count, places, splits),
            shapes,
            [smem()] + [vmem()] * (2 * subj_count),
            flops=len(places) * 4 * 10**8,
            limit=24,
            scratch=[pltpu.VMEM((len(places) * BLOCK, subj_count * lights * width), jnp.bfloat16)],
        )(code, *cols, *maps)

    blocks = list(range(blk_dev))
    to_far = mapped(code, [2 * blk_dev + b for b in blocks], (2,), (jnp.bfloat16,))
    from_far = []
    for h in range(2):
        from_far.append(swap_far(to_far[h]))
    code, _ = lax.optimization_barrier((code, to_far[0]))
    to_near, *own = mapped(code, [blk_dev + b for b in blocks] + blocks, (1, 2), (jnp.bfloat16, jnp.float32))
    from_near = swap_near(to_near)
    keep = far_real.astype(jnp.float32)

    subj_size = lax.axis_size("subj")
    distances = []
    while 2 ** len(distances) < subj_size:
        distances.append(2 ** len(distances))
    rows = frames // 2
    halves = []
    for h in range(2):
        mine_h = own[h]
        if h > 0:
            mine_h, halves[0] = lax.optimization_barrier((mine_h, halves[0]))
        near_h = from_near[h * rows : (h + 1) * rows].astype(jnp.float32)
        halves.append((mine_h + near_h + keep * from_far[h].astype(jnp.float32)).astype(jnp.bfloat16))
    for step in range(len(distances)):
        for h in range(2):
            sent = halves[h].astype(jnp.bfloat16)
            got = swap_subj(sent, distances[(step + h) % len(distances)])
            halves[h] = sent.astype(jnp.float32) + got.astype(jnp.float32)
    total = jnp.concatenate(halves, axis=0)
    return total / per_vertex[None, :] / (subj_count * subj_size)


def solution(mesh):
    def step(series, template, sl_blocks):
        in_specs = (P("subj", None, "cortex"), P(None, "cortex"), P("cortex", None))
        out_specs = P(None, "cortex")
        placed = jax.shard_map(body, mesh=mesh, in_specs=in_specs, out_specs=out_specs, check_vma=False)
        return placed(series, template, sl_blocks)

    return step
```

```python
import functools

import jax
import jax.numpy as jnp
from jax import lax
from jax.experimental import pallas as pl
from jax.experimental.pallas import tpu as pltpu
from jax.sharding import PartitionSpec as P


BLOCK = 128
NS_STEPS = 8
RIDGE_SHIFT = 0.1
NORM_EPSILON = 1e-06
COUNT_ROWS = 16
MIB = 1 << 20
LIMIT = 24


def swap_near(value):
    count = lax.axis_size("cortex")
    return lax.ppermute(value, "cortex", [(i, i ^ 1) for i in range(count)])


def swap_far(value):
    count = lax.axis_size("cortex")
    route = [(0, 0), (count - 1, count - 1)]
    for i in range(1, count - 1, 2):
        route += [(i, i + 1), (i + 1, i)]
    return lax.ppermute(value, "cortex", route)


def swap_subj(value, distance):
    count = lax.axis_size("subj")
    return lax.ppermute(value, "subj", [(i, i ^ distance) for i in range(count)])


def vmem():
    return pl.BlockSpec(memory_space=pltpu.VMEM)


def smem():
    return pl.BlockSpec(memory_space=pltpu.SMEM)


def call(kernel, out_shape, in_specs, flops, limit, scratch=()):
    outs = jax.tree.leaves(out_shape)
    return pl.pallas_call(
        kernel,
        out_shape=out_shape,
        in_specs=in_specs,
        out_specs=jax.tree.map(lambda _: vmem(), out_shape),
        scratch_shapes=list(scratch),
        compiler_params=pltpu.CompilerParams(vmem_limit_bytes=limit * MIB),
        cost_estimate=pl.CostEstimate(
            flops=flops, bytes_accessed=sum(o.size * o.dtype.itemsize for o in outs), transcendentals=0
        ),
    )


def columns(ref, half):
    return ref[:, pl.ds(pl.multiple_of(half * BLOCK, BLOCK), BLOCK)]


def template_kernel(code_ref, own_ref, near_ref, far_ref, out_ref):
    lights, members = code_ref.shape
    for g in range(lights):
        for j in range(members):
            code = code_ref[g, j]
            for place, ref in enumerate((own_ref, near_ref, far_ref)):

                @pl.when(code // 2 == place)
                def _():
                    out_ref[g, j * BLOCK : (j + 1) * BLOCK, :] = columns(ref, code % 2).T


def newton_schulz(now):
    head = now.shape[0] - BLOCK
    top, low = now[:head], now[head:]
    over = (((1,), (1,)), ((), ()))
    corner = lax.dot_general(top, top, over, preferred_element_type=jnp.float32).astype(jnp.bfloat16)
    bottom = lax.dot_general(low, now, over, preferred_element_type=jnp.float32).astype(jnp.bfloat16)
    gram = jnp.concatenate([jnp.concatenate([corner, bottom[:, :head].T], axis=1), bottom], axis=0)
    product = jnp.dot(gram, now, preferred_element_type=jnp.float32)
    return (1.5 * now.astype(jnp.float32) - 0.5 * product).astype(jnp.bfloat16)


def polar_kernel(subject, code_ref, tmpl_ref, own_ref, near_ref, far_ref, map_ref, cols_ref):
    lights, members = code_ref.shape
    width = members * BLOCK
    frames = own_ref.shape[0]
    for g in range(lights):
        for i in range(members):
            code = code_ref[g, i]
            lo = g * width + i * BLOCK
            for place, ref in enumerate((own_ref, near_ref.at[subject], far_ref)):

                @pl.when(code // 2 == place)
                def _():
                    cols_ref[:, lo : lo + BLOCK] = columns(ref, code % 2)

    row = lax.broadcasted_iota(jnp.int32, (width, width), 0)
    col = lax.broadcasted_iota(jnp.int32, (width, width), 1)
    ridge = jnp.where(row == col, RIDGE_SHIFT, 0.0)
    for g in range(lights):
        cross = jnp.dot(
            tmpl_ref[g], cols_ref[:, g * width : (g + 1) * width], preferred_element_type=jnp.float32
        )
        cross = cross * (1.0 / frames) + ridge
        squares = jnp.sum(cross * cross, keepdims=True)
        map_ref[g] = (cross * (1.0 / jnp.sqrt(squares + NORM_EPSILON))).astype(jnp.bfloat16)

    for _ in range(NS_STEPS):
        for g in range(lights):
            map_ref[g] = newton_schulz(map_ref[g])


def map_kernel(subj_count, places, splits, code_ref, *refs):
    cols_refs = refs[:subj_count]
    map_refs = refs[subj_count : 2 * subj_count]
    weight_ref = refs[-1]
    out_refs = refs[2 * subj_count : -1]
    lights, members = code_ref.shape
    width = members * BLOCK
    counts = []
    for p, place in enumerate(places):
        total = jnp.int32(0)
        for g in range(lights):
            pick = jnp.int32(0)
            found = code_ref[g, 0] == place
            for j in range(1, members):
                hit = code_ref[g, j] == place
                pick = jnp.where(hit, j, pick)
                found = jnp.logical_or(found, hit)
            total = total + found.astype(jnp.int32)
            rows = pl.ds(pl.multiple_of(pick * BLOCK, BLOCK), BLOCK)
            for s in range(subj_count):
                lo = (s * lights + g) * width
                piece = map_refs[s][g, rows, :]
                weight_ref[p * BLOCK : (p + 1) * BLOCK, lo : lo + width] = jnp.where(
                    found, piece, jnp.zeros_like(piece)
                )
        counts.append(total)
    depth = lights * width
    group = len(places) // len(splits)
    step_cols = group * BLOCK
    chunk = 256
    at = 0
    for n, pieces in enumerate(splits):
        first = n * step_cols
        weights = [
            weight_ref[first : first + step_cols, s * depth : (s + 1) * depth] for s in range(subj_count)
        ]
        rows = cols_refs[0].shape[0] // pieces
        for piece in range(pieces):
            for lo in range(0, rows, chunk):
                total = None
                for s in range(subj_count):
                    term = lax.dot_general(
                        cols_refs[s][piece * rows + lo : piece * rows + lo + chunk, :],
                        weights[s],
                        (((1,), (1,)), ((), ())),
                        preferred_element_type=jnp.float32,
                    )
                    total = term if total is None else total + term
                out_refs[at][lo : lo + chunk, :] = total.astype(out_refs[at].dtype)
            at += 1
        for b in range(group):
            tally = jnp.full((COUNT_ROWS, BLOCK), counts[n * group + b], jnp.int32)
            out_refs[at - 1][rows:, b * BLOCK : (b + 1) * BLOCK] = tally.astype(jnp.float32).astype(
                out_refs[at - 1].dtype
            )


def body(series, template, sl_blocks):
    subj_count, frames, width_dev = series.shape
    lights, members = sl_blocks.shape
    blk_dev = width_dev // BLOCK
    width = members * BLOCK
    count = lax.axis_size("cortex")
    position = lax.axis_index("cortex")
    odd = position % 2
    far_real = jnp.logical_and(position + 2 * odd - 1 >= 0, position + 2 * odd - 1 < count)

    tmpl_far = swap_far(template)
    tmpl_near = swap_near(template)
    parts = [series[s] for s in range(subj_count)]
    far = []
    for part in parts:
        far.append(swap_far(part))
    near = swap_near(series)

    window = sl_blocks - (position - 1) * blk_dev
    side = window // blk_dev
    place = jnp.where(side == 1, 0, jnp.where((side == 2) == (odd == 1), 2, 1))
    code = (place * blk_dev + window % blk_dev).astype(jnp.int32)

    tmpl_rows = call(
        template_kernel,
        jax.ShapeDtypeStruct((lights, width, frames), jnp.bfloat16),
        [smem(), vmem(), vmem(), vmem()],
        flops=10**9,
        limit=LIMIT,
    )(code, template, tmpl_near, tmpl_far)

    maps, cols = [], []
    for s in range(subj_count):
        polar, gathered = call(
            functools.partial(polar_kernel, s),
            (
                jax.ShapeDtypeStruct((lights, width, width), jnp.bfloat16),
                jax.ShapeDtypeStruct((frames, lights * width), jnp.bfloat16),
            ),
            [smem()] + [vmem()] * 4,
            flops=8 * 10**9,
            limit=LIMIT,
        )(code, tmpl_rows, parts[s], near, far[s])
        maps.append(polar)
        cols.append(gathered)

    def mapped(places, splits, types):
        shapes = [
            jax.ShapeDtypeStruct(
                (frames // pieces + (COUNT_ROWS if piece == pieces - 1 else 0), width_dev), kind
            )
            for pieces, kind in zip(splits, types)
            for piece in range(pieces)
        ]
        return call(
            functools.partial(map_kernel, subj_count, places, splits),
            shapes,
            [smem()] + [vmem()] * (2 * subj_count),
            flops=len(places) * 4 * 10**8,
            limit=LIMIT,
            scratch=[pltpu.VMEM((len(places) * BLOCK, subj_count * lights * width), jnp.bfloat16)],
        )(code, *cols, *maps)

    blocks = list(range(blk_dev))
    (to_far,) = mapped([2 * blk_dev + b for b in blocks], (1,), (jnp.bfloat16,))
    from_far = swap_far(to_far)
    code, _ = lax.optimization_barrier((code, to_far))
    to_near, *own = mapped([blk_dev + b for b in blocks] + blocks, (1, 2), (jnp.bfloat16, jnp.float32))
    from_near = swap_near(to_near)
    keep = far_real.astype(jnp.float32)

    def joined(mine, lo, hi):
        return mine + from_near[lo:hi].astype(jnp.float32) + keep * from_far[lo:hi].astype(jnp.float32)

    rows = frames // 2
    per_vertex = joined(own[1][rows : rows + 1], frames, frames + 1)
    halves = [joined(own[h][:rows], h * rows, (h + 1) * rows) for h in range(2)]
    subj_size = lax.axis_size("subj")
    distances = []
    while 2 ** len(distances) < subj_size:
        distances.append(2 ** len(distances))
    for step in range(len(distances)):
        for h in range(2):
            sent = halves[h].astype(jnp.bfloat16)
            got = swap_subj(sent, distances[(step + h) % len(distances)])
            halves[h] = sent.astype(jnp.float32) + got.astype(jnp.float32)
    total = jnp.concatenate(halves, axis=0)
    return total / per_vertex / (subj_count * subj_size)


def solution(mesh):
    def step(series, template, sl_blocks):
        in_specs = (P("subj", None, "cortex"), P(None, "cortex"), P("cortex", None))
        out_specs = P(None, "cortex")
        placed = jax.shard_map(body, mesh=mesh, in_specs=in_specs, out_specs=out_specs, check_vma=False)
        return placed(series, template, sl_blocks)

    return step
```

```python
import functools

import jax
import jax.numpy as jnp
from jax import lax
from jax.experimental import pallas as pl
from jax.experimental.pallas import tpu as pltpu
from jax.sharding import PartitionSpec as P


BLOCK = 128
NS_STEPS = 8
RIDGE_SHIFT = 0.1
NORM_EPSILON = 1e-06
COUNT_ROWS = 16
MIB = 1 << 20
LIMIT = 24
PIECES = 4


def swap_near(value):
    count = lax.axis_size("cortex")
    return lax.ppermute(value, "cortex", [(i, i ^ 1) for i in range(count)])


def swap_far(value):
    count = lax.axis_size("cortex")
    route = [(0, 0), (count - 1, count - 1)]
    for i in range(1, count - 1, 2):
        route += [(i, i + 1), (i + 1, i)]
    return lax.ppermute(value, "cortex", route)


def swap_subj(value, distance):
    count = lax.axis_size("subj")
    return lax.ppermute(value, "subj", [(i, i ^ distance) for i in range(count)])


def vmem():
    return pl.BlockSpec(memory_space=pltpu.VMEM)


def call(kernel, out_shape, in_specs, flops, limit, scratch=()):
    outs = jax.tree.leaves(out_shape)
    return pl.pallas_call(
        kernel,
        out_shape=out_shape,
        in_specs=in_specs,
        out_specs=jax.tree.map(lambda _: vmem(), out_shape),
        scratch_shapes=list(scratch),
        compiler_params=pltpu.CompilerParams(vmem_limit_bytes=limit * MIB),
        cost_estimate=pl.CostEstimate(
            flops=flops, bytes_accessed=sum(o.size * o.dtype.itemsize for o in outs), transcendentals=0
        ),
    )


def columns(ref, half):
    return ref[:, pl.ds(pl.multiple_of(half * BLOCK, BLOCK), BLOCK)]


def template_kernel(code_ref, own_ref, near_ref, far_ref, out_ref):
    lights, members = code_ref.shape
    for g in range(lights):
        for j in range(members):
            code = code_ref[g, j]
            for place, ref in enumerate((own_ref, near_ref, far_ref)):

                @pl.when(code // 2 == place)
                def _():
                    out_ref[g, j * BLOCK : (j + 1) * BLOCK, :] = columns(ref, code % 2).T


def newton_schulz(now_ref, next_ref, gram_ref):
    lights, width, _ = now_ref.shape
    head = width - BLOCK
    over = (((1,), (1,)), ((), ()))
    for g in range(lights):
        top = now_ref[g, :head]
        corner = lax.dot_general(top, top, over, preferred_element_type=jnp.float32)
        gram_ref[g, :head, :head] = corner.astype(jnp.bfloat16)
        low = lax.dot_general(now_ref[g, head:], now_ref[g], over, preferred_element_type=jnp.float32)
        low = low.astype(jnp.bfloat16)
        gram_ref[g, head:, :] = low
        gram_ref[g, :head, head:] = low[:, :head].T
    for g in range(lights):
        now = now_ref[g]
        product = jnp.dot(gram_ref[g], now, preferred_element_type=jnp.float32)
        next_ref[g] = (1.5 * now.astype(jnp.float32) - 0.5 * product).astype(jnp.bfloat16)


def polar_kernel(subject, code_ref, tmpl_ref, own_ref, near_ref, far_ref, map_ref, cols_ref, odd_ref, gram_ref):
    lights, members = code_ref.shape
    width = members * BLOCK
    frames = own_ref.shape[0]
    for g in range(lights):
        for i in range(members):
            code = code_ref[g, i]
            lo = g * width + i * BLOCK
            for place, ref in enumerate((own_ref, near_ref.at[subject], far_ref)):

                @pl.when(code // 2 == place)
                def _():
                    cols_ref[:, lo : lo + BLOCK] = columns(ref, code % 2)

    first_ref = map_ref if NS_STEPS % 2 == 0 else odd_ref
    row = lax.broadcasted_iota(jnp.int32, (width, width), 0)
    col = lax.broadcasted_iota(jnp.int32, (width, width), 1)
    ridge = jnp.where(row == col, RIDGE_SHIFT, 0.0)
    for g in range(lights):
        cross = jnp.dot(
            tmpl_ref[g], cols_ref[:, g * width : (g + 1) * width], preferred_element_type=jnp.float32
        )
        cross = cross * (1.0 / frames) + ridge
        squares = jnp.sum(cross * cross, keepdims=True)
        first_ref[g] = (cross * (1.0 / jnp.sqrt(squares + NORM_EPSILON))).astype(jnp.bfloat16)

    turns = (first_ref, odd_ref if first_ref is map_ref else map_ref)
    for step in range(NS_STEPS):
        newton_schulz(turns[step % 2], turns[1 - step % 2], gram_ref)


def map_kernel(subj_count, places, splits, code_ref, *refs):
    cols_refs = refs[:subj_count]
    map_refs = refs[subj_count : 2 * subj_count]
    weight_ref = refs[-1]
    out_refs = refs[2 * subj_count : -1]
    lights, members = code_ref.shape
    width = members * BLOCK
    counts = []
    for p, place in enumerate(places):
        total = jnp.int32(0)
        for g in range(lights):
            pick = jnp.int32(0)
            found = code_ref[g, 0] == place
            for j in range(1, members):
                hit = code_ref[g, j] == place
                pick = jnp.where(hit, j, pick)
                found = jnp.logical_or(found, hit)
            total = total + found.astype(jnp.int32)
            rows = pl.ds(pl.multiple_of(pick * BLOCK, BLOCK), BLOCK)
            for s in range(subj_count):
                lo = (s * lights + g) * width
                piece = map_refs[s][g, rows, :]
                weight_ref[p * BLOCK : (p + 1) * BLOCK, lo : lo + width] = jnp.where(
                    found, piece, jnp.zeros_like(piece)
                )
        counts.append(total)
    depth = lights * width
    group = len(places) // len(splits)
    step_cols = group * BLOCK
    chunk = 256
    at = 0
    for n, pieces in enumerate(splits):
        first = n * step_cols
        weights = [
            weight_ref[first : first + step_cols, s * depth : (s + 1) * depth] for s in range(subj_count)
        ]
        rows = cols_refs[0].shape[0] // pieces
        for piece in range(pieces):
            for lo in range(0, rows, chunk):
                total = None
                for s in range(subj_count):
                    term = lax.dot_general(
                        cols_refs[s][piece * rows + lo : piece * rows + lo + chunk, :],
                        weights[s],
                        (((1,), (1,)), ((), ())),
                        preferred_element_type=jnp.float32,
                    )
                    total = term if total is None else total + term
                out_refs[at][lo : lo + chunk, :] = total.astype(out_refs[at].dtype)
            at += 1
        for b in range(group):
            tally = jnp.full((COUNT_ROWS, BLOCK), counts[n * group + b], jnp.int32)
            out_refs[at - 1][rows:, b * BLOCK : (b + 1) * BLOCK] = tally.astype(jnp.float32).astype(
                out_refs[at - 1].dtype
            )


def body(series, template, sl_blocks):
    subj_count, frames, width_dev = series.shape
    lights, members = sl_blocks.shape
    blk_dev = width_dev // BLOCK
    width = members * BLOCK
    count = lax.axis_size("cortex")
    position = lax.axis_index("cortex")
    odd = position % 2
    far_real = jnp.logical_and(position + 2 * odd - 1 >= 0, position + 2 * odd - 1 < count)

    tmpl_far = swap_far(template)
    tmpl_near = swap_near(template)
    parts = [series[s] for s in range(subj_count)]
    far = []
    for part in parts:
        far.append(swap_far(part))
    near = swap_near(series)

    window = sl_blocks - (position - 1) * blk_dev
    side = window // blk_dev
    place = jnp.where(side == 1, 0, jnp.where((side == 2) == (odd == 1), 2, 1))
    code = (place * blk_dev + window % blk_dev).astype(jnp.int32)

    tmpl_rows = call(
        template_kernel,
        jax.ShapeDtypeStruct((lights, width, frames), jnp.bfloat16),
        [vmem()] * 4,
        flops=10**9,
        limit=LIMIT,
    )(code, template, tmpl_near, tmpl_far)

    maps, cols = [], []
    for s in range(subj_count):
        polar, gathered = call(
            functools.partial(polar_kernel, s),
            (
                jax.ShapeDtypeStruct((lights, width, width), jnp.bfloat16),
                jax.ShapeDtypeStruct((frames, lights * width), jnp.bfloat16),
            ),
            [vmem()] * 5,
            flops=8 * 10**9,
            limit=LIMIT,
            scratch=[pltpu.VMEM((lights, width, width), jnp.bfloat16)] * 2,
        )(code, tmpl_rows, parts[s], near, far[s])
        maps.append(polar)
        cols.append(gathered)

    def mapped(places, splits, types):
        shapes = [
            jax.ShapeDtypeStruct(
                (frames // pieces + (COUNT_ROWS if piece == pieces - 1 else 0), width_dev), kind
            )
            for pieces, kind in zip(splits, types)
            for piece in range(pieces)
        ]
        return call(
            functools.partial(map_kernel, subj_count, places, splits),
            shapes,
            [vmem()] * (1 + 2 * subj_count),
            flops=len(places) * 4 * 10**8,
            limit=LIMIT,
            scratch=[pltpu.VMEM((len(places) * BLOCK, subj_count * lights * width), jnp.bfloat16)],
        )(code, *cols, *maps)

    blocks = list(range(blk_dev))
    (to_far,) = mapped([2 * blk_dev + b for b in blocks], (1,), (jnp.bfloat16,))
    from_far = swap_far(to_far)
    code, _ = lax.optimization_barrier((code, to_far))
    to_near, *own = mapped([blk_dev + b for b in blocks] + blocks, (1, PIECES), (jnp.bfloat16, jnp.float32))
    from_near = swap_near(to_near)
    keep = far_real.astype(jnp.float32)

    def joined(mine, lo, hi):
        return mine + from_near[lo:hi].astype(jnp.float32) + keep * from_far[lo:hi].astype(jnp.float32)

    rows = frames // PIECES
    per_vertex = joined(own[-1][rows : rows + 1], frames, frames + 1)
    halves = [joined(own[h][:rows], h * rows, (h + 1) * rows) for h in range(PIECES)]
    subj_size = lax.axis_size("subj")
    distances = []
    while 2 ** len(distances) < subj_size:
        distances.append(2 ** len(distances))
    for step in range(len(distances)):
        for h in range(PIECES):
            sent = halves[h].astype(jnp.bfloat16)
            got = swap_subj(sent, distances[(step + h) % len(distances)])
            halves[h] = sent.astype(jnp.float32) + got.astype(jnp.float32)
    total = jnp.concatenate(halves, axis=0)
    return total / per_vertex / (subj_count * subj_size)


def solution(mesh):
    def step(series, template, sl_blocks):
        in_specs = (P("subj", None, "cortex"), P(None, "cortex"), P("cortex", None))
        out_specs = P(None, "cortex")
        placed = jax.shard_map(body, mesh=mesh, in_specs=in_specs, out_specs=out_specs, check_vma=False)
        return placed(series, template, sl_blocks)

    return step
```

```python
import functools

import jax
import jax.numpy as jnp
from jax import lax
from jax.experimental import pallas as pl
from jax.experimental.pallas import tpu as pltpu
from jax.sharding import PartitionSpec as P


BLOCK = 128
NS_STEPS = 8
RIDGE_SHIFT = 0.1
NORM_EPSILON = 1e-06
COUNT_ROWS = 16
MIB = 1 << 20
LIMIT = 24
PIECES = 4


def swap_near(value):
    count = lax.axis_size("cortex")
    return lax.ppermute(value, "cortex", [(i, i ^ 1) for i in range(count)])


def swap_far(value):
    count = lax.axis_size("cortex")
    route = [(0, 0), (count - 1, count - 1)]
    for i in range(1, count - 1, 2):
        route += [(i, i + 1), (i + 1, i)]
    return lax.ppermute(value, "cortex", route)


def swap_subj(value, distance):
    count = lax.axis_size("subj")
    return lax.ppermute(value, "subj", [(i, i ^ distance) for i in range(count)])


def vmem():
    return pl.BlockSpec(memory_space=pltpu.VMEM)


def call(kernel, out_shape, in_specs, flops, limit, scratch=()):
    outs = jax.tree.leaves(out_shape)
    return pl.pallas_call(
        kernel,
        out_shape=out_shape,
        in_specs=in_specs,
        out_specs=jax.tree.map(lambda _: vmem(), out_shape),
        scratch_shapes=list(scratch),
        compiler_params=pltpu.CompilerParams(vmem_limit_bytes=limit * MIB),
        cost_estimate=pl.CostEstimate(
            flops=flops, bytes_accessed=sum(o.size * o.dtype.itemsize for o in outs), transcendentals=0
        ),
    )


def columns(ref, half):
    return ref[:, pl.ds(pl.multiple_of(half * BLOCK, BLOCK), BLOCK)]


def template_kernel(code_ref, own_ref, near_ref, far_ref, out_ref):
    lights, members = code_ref.shape
    for g in range(lights):
        for j in range(members):
            code = code_ref[g, j]
            for place, ref in enumerate((own_ref, near_ref, far_ref)):

                @pl.when(code // 2 == place)
                def _():
                    out_ref[g, j * BLOCK : (j + 1) * BLOCK, :] = columns(ref, code % 2).T


def newton_schulz(now_ref, next_ref, gram_ref):
    lights, width, _ = now_ref.shape
    head = width - BLOCK
    over = (((1,), (1,)), ((), ()))
    for g in range(lights):
        top = now_ref[g, :head]
        corner = lax.dot_general(top, top, over, preferred_element_type=jnp.float32)
        gram_ref[g, :head, :head] = corner.astype(jnp.bfloat16)
        low = lax.dot_general(now_ref[g, head:], now_ref[g], over, preferred_element_type=jnp.float32)
        low = low.astype(jnp.bfloat16)
        gram_ref[g, head:, :] = low
        gram_ref[g, :head, head:] = low[:, :head].T
    for g in range(lights):
        now = now_ref[g]
        product = jnp.dot(gram_ref[g, :, :head], now[:head], preferred_element_type=jnp.float32)
        product += jnp.dot(gram_ref[g, :, head:], now[head:], preferred_element_type=jnp.float32)
        next_ref[g] = (1.5 * now.astype(jnp.float32) - 0.5 * product).astype(jnp.bfloat16)


def polar_kernel(subject, code_ref, tmpl_ref, own_ref, near_ref, far_ref, map_ref, cols_ref, odd_ref, gram_ref, *stage):
    lights, members = code_ref.shape
    width = members * BLOCK
    frames = own_ref.shape[0]
    arrival = None
    if stage:
        staged_ref, arrived = stage
        arrival = pltpu.make_async_copy(far_ref, staged_ref, arrived)
        arrival.start()
        far_ref = staged_ref

    def gather(sources):
        for g in range(lights):
            for i in range(members):
                code = code_ref[g, i]
                lo = g * width + i * BLOCK
                for place, ref in sources:

                    @pl.when(code // 2 == place)
                    def _():
                        cols_ref[:, lo : lo + BLOCK] = columns(ref, code % 2)

    gather(((0, own_ref), (1, near_ref.at[subject])))
    if arrival is not None:
        arrival.wait()
    gather(((2, far_ref),))

    first_ref = map_ref if NS_STEPS % 2 == 0 else odd_ref
    row = lax.broadcasted_iota(jnp.int32, (width, width), 0)
    col = lax.broadcasted_iota(jnp.int32, (width, width), 1)
    ridge = jnp.where(row == col, RIDGE_SHIFT, 0.0)
    for g in range(lights):
        cross = jnp.dot(
            tmpl_ref[g], cols_ref[:, g * width : (g + 1) * width], preferred_element_type=jnp.float32
        )
        cross = cross * (1.0 / frames) + ridge
        squares = jnp.sum(cross * cross, keepdims=True)
        first_ref[g] = (cross * (1.0 / jnp.sqrt(squares + NORM_EPSILON))).astype(jnp.bfloat16)

    turns = (first_ref, odd_ref if first_ref is map_ref else map_ref)
    for step in range(NS_STEPS):
        newton_schulz(turns[step % 2], turns[1 - step % 2], gram_ref)


def map_kernel(subj_count, places, splits, code_ref, *refs):
    cols_refs = refs[:subj_count]
    map_refs = refs[subj_count : 2 * subj_count]
    weight_ref = refs[-1]
    out_refs = refs[2 * subj_count : -1]
    lights, members = code_ref.shape
    width = members * BLOCK
    counts = []
    for p, place in enumerate(places):
        total = jnp.int32(0)
        for g in range(lights):
            pick = jnp.int32(0)
            found = code_ref[g, 0] == place
            for j in range(1, members):
                hit = code_ref[g, j] == place
                pick = jnp.where(hit, j, pick)
                found = jnp.logical_or(found, hit)
            total = total + found.astype(jnp.int32)
            rows = pl.ds(pl.multiple_of(pick * BLOCK, BLOCK), BLOCK)
            for s in range(subj_count):
                lo = (s * lights + g) * width
                piece = map_refs[s][g, rows, :]
                weight_ref[p * BLOCK : (p + 1) * BLOCK, lo : lo + width] = jnp.where(
                    found, piece, jnp.zeros_like(piece)
                )
        counts.append(total)
    depth = lights * width
    group = len(places) // len(splits)
    step_cols = group * BLOCK
    chunk = 256
    at = 0
    for n, pieces in enumerate(splits):
        first = n * step_cols
        weights = [
            weight_ref[first : first + step_cols, s * depth : (s + 1) * depth] for s in range(subj_count)
        ]
        for b in range(group):
            tally = jnp.full((COUNT_ROWS, BLOCK), counts[n * group + b], jnp.int32)
            out_refs[at][pieces[0] :, b * BLOCK : (b + 1) * BLOCK] = tally.astype(jnp.float32).astype(
                out_refs[at].dtype
            )
        above = 0
        for rows in pieces:
            for lo in range(0, rows, chunk):
                total = None
                for s in range(subj_count):
                    term = lax.dot_general(
                        cols_refs[s][above + lo : above + lo + chunk, :],
                        weights[s],
                        (((1,), (1,)), ((), ())),
                        preferred_element_type=jnp.float32,
                    )
                    total = term if total is None else total + term
                out_refs[at][lo : lo + chunk, :] = total.astype(out_refs[at].dtype)
            above += rows
            at += 1


def body(series, template, sl_blocks):
    subj_count, frames, width_dev = series.shape
    lights, members = sl_blocks.shape
    blk_dev = width_dev // BLOCK
    width = members * BLOCK
    count = lax.axis_size("cortex")
    position = lax.axis_index("cortex")
    odd = position % 2
    far_real = jnp.logical_and(position + 2 * odd - 1 >= 0, position + 2 * odd - 1 < count)

    tmpl_far = swap_far(template)
    tmpl_near = swap_near(template)
    parts = [series[s] for s in range(subj_count)]
    far = []
    for part in parts:
        far.append(swap_far(part))
    near = swap_near(series)

    window = sl_blocks - (position - 1) * blk_dev
    side = window // blk_dev
    place = jnp.where(side == 1, 0, jnp.where((side == 2) == (odd == 1), 2, 1))
    code = (place * blk_dev + window % blk_dev).astype(jnp.int32)

    tmpl_rows = call(
        template_kernel,
        jax.ShapeDtypeStruct((lights, width, frames), jnp.bfloat16),
        [vmem()] * 4,
        flops=10**9,
        limit=LIMIT,
    )(code, template, tmpl_near, tmpl_far)

    maps, cols = [], []
    for s in range(subj_count):
        polar, gathered = call(
            functools.partial(polar_kernel, s),
            (
                jax.ShapeDtypeStruct((lights, width, width), jnp.bfloat16),
                jax.ShapeDtypeStruct((frames, lights * width), jnp.bfloat16),
            ),
            [vmem()] * 4 + [pl.BlockSpec(memory_space=pl.ANY) if s > 0 else vmem()],
            flops=8 * 10**9,
            limit=LIMIT,
            scratch=[pltpu.VMEM((lights, width, width), jnp.bfloat16)] * 2
            + ([pltpu.VMEM((frames, width_dev), jnp.bfloat16), pltpu.SemaphoreType.DMA] if s > 0 else []),
        )(code, tmpl_rows, parts[s], near, far[s])
        maps.append(polar)
        cols.append(gathered)

    def mapped(places, splits, types):
        shapes = [
            jax.ShapeDtypeStruct((rows + (COUNT_ROWS if n == 0 else 0), width_dev), kind)
            for pieces, kind in zip(splits, types)
            for n, rows in enumerate(pieces)
        ]
        return call(
            functools.partial(map_kernel, subj_count, places, splits),
            shapes,
            [vmem()] * (1 + 2 * subj_count),
            flops=len(places) * 4 * 10**8,
            limit=LIMIT,
            scratch=[pltpu.VMEM((len(places) * BLOCK, subj_count * lights * width), jnp.bfloat16)],
        )(code, *cols, *maps)

    subj_size = lax.axis_size("subj")
    distances = subject_distances(subj_size)
    rows = frames // PIECES
    late = frames - rows
    blocks = list(range(blk_dev))

    def swapped(value, step, turn):
        got = swap_subj(value, distances[(step + turn) % len(distances)])
        return value.astype(jnp.float32) + got.astype(jnp.float32)

    to_far, early_far = mapped([2 * blk_dev + b for b in blocks], ((late, rows),), (jnp.bfloat16,))
    from_far = swap_far(to_far)
    code, _ = lax.optimization_barrier((code, to_far))
    to_near, *own = mapped(
        [blk_dev + b for b in blocks] + blocks, ((frames,), (rows,) * PIECES), (jnp.bfloat16, jnp.float32)
    )
    from_near = swap_near(to_near)
    early_own = own[-1] + from_near[late:frames].astype(jnp.float32)
    early_own, from_near = lax.optimization_barrier((early_own.astype(jnp.bfloat16), from_near))
    keep = far_real.astype(jnp.float32)

    def joined(mine, lo, far_lo, size):
        near_rows = from_near[lo : lo + size].astype(jnp.float32)
        return mine + near_rows + keep * from_far[far_lo : far_lo + size].astype(jnp.float32)

    per_vertex = joined(own[0][rows : rows + 1], frames, late, 1)
    parts = [joined(own[h][:rows], h * rows, h * rows, rows) for h in range(PIECES - 1)]
    for step in range(len(distances)):
        early_own = swapped(early_own.astype(jnp.bfloat16), step, 1)
        early_far = swapped(early_far.astype(jnp.bfloat16), step, 0)
        parts = [swapped(p.astype(jnp.bfloat16), step, h) for h, p in enumerate(parts)]
    early_back = swap_far(early_far.astype(jnp.bfloat16))
    parts.append(early_own + keep * early_back.astype(jnp.float32))
    return jnp.concatenate(parts, axis=0) / per_vertex / (subj_count * subj_size)


def subject_distances(size):
    distances = []
    while 2 ** len(distances) < size:
        distances.append(2 ** len(distances))
    return distances


def solution(mesh):
    def step(series, template, sl_blocks):
        in_specs = (P("subj", None, "cortex"), P(None, "cortex"), P("cortex", None))
        out_specs = P(None, "cortex")
        placed = jax.shard_map(body, mesh=mesh, in_specs=in_specs, out_specs=out_specs, check_vma=False)
        return placed(series, template, sl_blocks)

    return step
```

```python
import functools

import jax
import jax.numpy as jnp
from jax import lax
from jax.experimental import pallas as pl
from jax.experimental.pallas import tpu as pltpu
from jax.sharding import PartitionSpec as P


BLOCK = 128
NS_STEPS = 8
RIDGE_SHIFT = 0.1
NORM_EPSILON = 1e-06
COUNT_ROWS = 16
MIB = 1 << 20
LIMIT = 24
PIECES = 4


def swap_near(value):
    count = lax.axis_size("cortex")
    return lax.ppermute(value, "cortex", [(i, i ^ 1) for i in range(count)])


def swap_far(value):
    count = lax.axis_size("cortex")
    route = [(0, 0), (count - 1, count - 1)]
    for i in range(1, count - 1, 2):
        route += [(i, i + 1), (i + 1, i)]
    return lax.ppermute(value, "cortex", route)


def swap_subj(value, distance):
    count = lax.axis_size("subj")
    return lax.ppermute(value, "subj", [(i, i ^ distance) for i in range(count)])


def vmem():
    return pl.BlockSpec(memory_space=pltpu.VMEM)


def call(kernel, out_shape, in_specs, flops, limit, scratch=()):
    outs = jax.tree.leaves(out_shape)
    return pl.pallas_call(
        kernel,
        out_shape=out_shape,
        in_specs=in_specs,
        out_specs=jax.tree.map(lambda _: vmem(), out_shape),
        scratch_shapes=list(scratch),
        compiler_params=pltpu.CompilerParams(vmem_limit_bytes=limit * MIB),
        cost_estimate=pl.CostEstimate(
            flops=flops, bytes_accessed=sum(o.size * o.dtype.itemsize for o in outs), transcendentals=0
        ),
    )


def read_codes(code_ref):
    lights, members = code_ref.shape
    return [[code_ref[g, j] for j in range(members)] for g in range(lights)]


def columns(ref, half):
    return ref[:, pl.ds(pl.multiple_of(half * BLOCK, BLOCK), BLOCK)]


def template_kernel(code_ref, own_ref, near_ref, far_ref, out_ref):
    lights, members = code_ref.shape
    codes = read_codes(code_ref)
    for g in range(lights):
        for j in range(members):
            code = codes[g][j]
            for place, ref in enumerate((own_ref, near_ref, far_ref)):

                @pl.when(code // 2 == place)
                def _():
                    out_ref[g, j * BLOCK : (j + 1) * BLOCK, :] = columns(ref, code % 2).T


def newton_schulz(now_ref, next_ref, gram_ref):
    lights, width, _ = now_ref.shape
    head = width - BLOCK
    over = (((1,), (1,)), ((), ()))
    for g in range(lights):
        top = now_ref[g, :head]
        corner = lax.dot_general(top, top, over, preferred_element_type=jnp.float32)
        gram_ref[g, :head, :head] = corner.astype(jnp.bfloat16)
        low = lax.dot_general(now_ref[g, head:], now_ref[g], over, preferred_element_type=jnp.float32)
        low = low.astype(jnp.bfloat16)
        gram_ref[g, head:, :] = low
        gram_ref[g, :head, head:] = low[:, :head].T
    for g in range(lights):
        now = now_ref[g]
        product = jnp.dot(gram_ref[g, :, :head], now[:head], preferred_element_type=jnp.float32)
        product += jnp.dot(gram_ref[g, :, head:], now[head:], preferred_element_type=jnp.float32)
        next_ref[g] = (1.5 * now.astype(jnp.float32) - 0.5 * product).astype(jnp.bfloat16)


def polar_kernel(subject, code_ref, tmpl_ref, own_ref, near_ref, far_ref, map_ref, cols_ref, odd_ref, gram_ref, *stage):
    lights, members = code_ref.shape
    width = members * BLOCK
    frames = own_ref.shape[0]
    codes = read_codes(code_ref)
    arrival = None
    if stage:
        staged_ref, arrived = stage
        arrival = pltpu.make_async_copy(far_ref, staged_ref, arrived)
        arrival.start()
        far_ref = staged_ref

    def gather(sources):
        for g in range(lights):
            for i in range(members):
                code = codes[g][i]
                lo = g * width + i * BLOCK
                for place, ref in sources:

                    @pl.when(code // 2 == place)
                    def _():
                        cols_ref[:, lo : lo + BLOCK] = columns(ref, code % 2)

    gather(((0, own_ref), (1, near_ref.at[subject])))
    if arrival is not None:
        arrival.wait()
    gather(((2, far_ref),))

    first_ref = map_ref if NS_STEPS % 2 == 0 else odd_ref
    row = lax.broadcasted_iota(jnp.int32, (width, width), 0)
    col = lax.broadcasted_iota(jnp.int32, (width, width), 1)
    ridge = jnp.where(row == col, RIDGE_SHIFT, 0.0)
    for g in range(lights):
        cross = jnp.dot(
            tmpl_ref[g], cols_ref[:, g * width : (g + 1) * width], preferred_element_type=jnp.float32
        )
        cross = cross * (1.0 / frames) + ridge
        squares = jnp.sum(cross * cross, keepdims=True)
        first_ref[g] = (cross * (1.0 / jnp.sqrt(squares + NORM_EPSILON))).astype(jnp.bfloat16)

    turns = (first_ref, odd_ref if first_ref is map_ref else map_ref)
    for step in range(NS_STEPS):
        newton_schulz(turns[step % 2], turns[1 - step % 2], gram_ref)


def map_kernel(subj_count, places, splits, code_ref, *refs):
    cols_refs = refs[:subj_count]
    map_refs = refs[subj_count : 2 * subj_count]
    weight_ref = refs[-1]
    out_refs = refs[2 * subj_count : -1]
    lights, members = code_ref.shape
    width = members * BLOCK
    codes = read_codes(code_ref)
    counts = []
    for p, place in enumerate(places):
        total = jnp.int32(0)
        for g in range(lights):
            pick = jnp.int32(0)
            found = codes[g][0] == place
            for j in range(1, members):
                hit = codes[g][j] == place
                pick = jnp.where(hit, j, pick)
                found = jnp.logical_or(found, hit)
            total = total + found.astype(jnp.int32)
            rows = pl.ds(pl.multiple_of(pick * BLOCK, BLOCK), BLOCK)
            for s in range(subj_count):
                lo = (s * lights + g) * width
                piece = map_refs[s][g, rows, :]
                weight_ref[p * BLOCK : (p + 1) * BLOCK, lo : lo + width] = jnp.where(
                    found, piece, jnp.zeros_like(piece)
                )
        counts.append(total)
    depth = lights * width
    group = len(places) // len(splits)
    step_cols = group * BLOCK
    chunk = 256
    at = 0
    for n, pieces in enumerate(splits):
        first = n * step_cols
        weights = [
            weight_ref[first : first + step_cols, s * depth : (s + 1) * depth] for s in range(subj_count)
        ]
        for b in range(group):
            tally = jnp.full((COUNT_ROWS, BLOCK), counts[n * group + b], jnp.int32)
            out_refs[at][pieces[0] :, b * BLOCK : (b + 1) * BLOCK] = tally.astype(jnp.float32).astype(
                out_refs[at].dtype
            )
        above = 0
        for rows in pieces:
            for lo in range(0, rows, chunk):
                total = None
                for s in range(subj_count):
                    term = lax.dot_general(
                        cols_refs[s][above + lo : above + lo + chunk, :],
                        weights[s],
                        (((1,), (1,)), ((), ())),
                        preferred_element_type=jnp.float32,
                    )
                    total = term if total is None else total + term
                out_refs[at][lo : lo + chunk, :] = total.astype(out_refs[at].dtype)
            above += rows
            at += 1


def finish_kernel(subjects, sent_ref, got_ref, cover_ref, *rest):
    total = sent_ref[...].astype(jnp.float32) + got_ref[...].astype(jnp.float32)
    rest[-1][...] = total / cover_ref[...] / subjects


def finished(result, piece, pair, cover, subjects):
    rows, cols = pair[0].shape
    placed = [] if result is None else [result]
    return pl.pallas_call(
        functools.partial(finish_kernel, subjects),
        out_shape=jax.ShapeDtypeStruct((rows * PIECES, cols), jnp.float32),
        in_specs=[vmem()] * 3 + [pl.BlockSpec(memory_space=pl.ANY)] * len(placed),
        out_specs=pl.BlockSpec((rows, cols), lambda i: (piece, 0)),
        grid=(1,),
        input_output_aliases={3: 0} if placed else {},
        compiler_params=pltpu.CompilerParams(vmem_limit_bytes=LIMIT * MIB),
        name="finish",
    )(*pair, cover, *placed)


def body(series, template, sl_blocks):
    subj_count, frames, width_dev = series.shape
    lights, members = sl_blocks.shape
    blk_dev = width_dev // BLOCK
    width = members * BLOCK
    count = lax.axis_size("cortex")
    position = lax.axis_index("cortex")
    odd = position % 2
    far_real = jnp.logical_and(position + 2 * odd - 1 >= 0, position + 2 * odd - 1 < count)

    tmpl_far = swap_far(template)
    tmpl_near = swap_near(template)
    parts = [series[s] for s in range(subj_count)]
    far = []
    for part in parts:
        far.append(swap_far(part))
    near = swap_near(series)

    window = sl_blocks - (position - 1) * blk_dev
    side = window // blk_dev
    place = jnp.where(side == 1, 0, jnp.where((side == 2) == (odd == 1), 2, 1))
    code = (place * blk_dev + window % blk_dev).astype(jnp.int32)

    tmpl_rows = call(
        template_kernel,
        jax.ShapeDtypeStruct((lights, width, frames), jnp.bfloat16),
        [vmem()] * 4,
        flops=10**9,
        limit=LIMIT,
    )(code, template, tmpl_near, tmpl_far)

    maps, cols = [], []
    for s in range(subj_count):
        polar, gathered = call(
            functools.partial(polar_kernel, s),
            (
                jax.ShapeDtypeStruct((lights, width, width), jnp.bfloat16),
                jax.ShapeDtypeStruct((frames, lights * width), jnp.bfloat16),
            ),
            [vmem()] * 4 + [pl.BlockSpec(memory_space=pl.ANY) if s > 0 else vmem()],
            flops=8 * 10**9,
            limit=LIMIT,
            scratch=[pltpu.VMEM((lights, width, width), jnp.bfloat16)] * 2
            + ([pltpu.VMEM((frames, width_dev), jnp.bfloat16), pltpu.SemaphoreType.DMA] if s > 0 else []),
        )(code, tmpl_rows, parts[s], near, far[s])
        maps.append(polar)
        cols.append(gathered)

    def mapped(places, splits, types):
        shapes = [
            jax.ShapeDtypeStruct((rows + (COUNT_ROWS if n == 0 else 0), width_dev), kind)
            for pieces, kind in zip(splits, types)
            for n, rows in enumerate(pieces)
        ]
        return call(
            functools.partial(map_kernel, subj_count, places, splits),
            shapes,
            [vmem()] * (1 + 2 * subj_count),
            flops=len(places) * 4 * 10**8,
            limit=LIMIT,
            scratch=[pltpu.VMEM((len(places) * BLOCK, subj_count * lights * width), jnp.bfloat16)],
        )(code, *cols, *maps)

    blocks = list(range(blk_dev))
    (to_far,) = mapped([2 * blk_dev + b for b in blocks], ((frames,),), (jnp.bfloat16,))
    from_far = swap_far(to_far)
    code, _ = lax.optimization_barrier((code, to_far))
    to_near, *own = mapped(
        [blk_dev + b for b in blocks] + blocks, ((frames,), (frames // PIECES,) * PIECES), (jnp.bfloat16, jnp.float32)
    )
    from_near = swap_near(to_near)
    keep = far_real.astype(jnp.float32)

    def joined(mine, lo, hi):
        return mine + from_near[lo:hi].astype(jnp.float32) + keep * from_far[lo:hi].astype(jnp.float32)

    rows = frames // PIECES
    per_vertex = joined(own[0][rows : rows + 1], frames, frames + 1)
    halves = [joined(own[h][:rows], h * rows, (h + 1) * rows) for h in range(PIECES)]
    subj_size = lax.axis_size("subj")
    distances = []
    while 2 ** len(distances) < subj_size:
        distances.append(2 ** len(distances))
    pairs = []
    for step in range(len(distances)):
        pairs = []
        for h in range(PIECES):
            sent = halves[h].astype(jnp.bfloat16)
            got = swap_subj(sent, distances[(step + h) % len(distances)])
            halves[h] = sent.astype(jnp.float32) + got.astype(jnp.float32)
            pairs.append((sent, got))
    if not pairs:
        return jnp.concatenate(halves, axis=0) / per_vertex / (subj_count * subj_size)
    result = None
    for h, pair in enumerate(pairs):
        result = finished(result, h, pair, per_vertex, subj_count * subj_size)
    return result


def solution(mesh):
    def step(series, template, sl_blocks):
        in_specs = (P("subj", None, "cortex"), P(None, "cortex"), P("cortex", None))
        out_specs = P(None, "cortex")
        placed = jax.shard_map(body, mesh=mesh, in_specs=in_specs, out_specs=out_specs, check_vma=False)
        return placed(series, template, sl_blocks)

    return step
```

```python
import functools

import jax
import jax.numpy as jnp
from jax import lax
from jax.experimental import pallas as pl
from jax.experimental.pallas import tpu as pltpu
from jax.sharding import PartitionSpec as P


BLOCK = 128
NS_STEPS = 8
RIDGE_SHIFT = 0.1
NORM_EPSILON = 1e-06
COUNT_ROWS = 16
MIB = 1 << 20
LIMIT = 24
PIECES = 4


def swap_near(value):
    count = lax.axis_size("cortex")
    return lax.ppermute(value, "cortex", [(i, i ^ 1) for i in range(count)])


def swap_far(value):
    count = lax.axis_size("cortex")
    route = [(0, 0), (count - 1, count - 1)]
    for i in range(1, count - 1, 2):
        route += [(i, i + 1), (i + 1, i)]
    return lax.ppermute(value, "cortex", route)


def swap_subj(value, distance):
    count = lax.axis_size("subj")
    return lax.ppermute(value, "subj", [(i, i ^ distance) for i in range(count)])


def vmem():
    return pl.BlockSpec(memory_space=pltpu.VMEM)


def call(kernel, out_shape, in_specs, flops, limit, scratch=()):
    outs = jax.tree.leaves(out_shape)
    return pl.pallas_call(
        kernel,
        out_shape=out_shape,
        in_specs=in_specs,
        out_specs=jax.tree.map(lambda _: vmem(), out_shape),
        scratch_shapes=list(scratch),
        compiler_params=pltpu.CompilerParams(vmem_limit_bytes=limit * MIB),
        cost_estimate=pl.CostEstimate(
            flops=flops, bytes_accessed=sum(o.size * o.dtype.itemsize for o in outs), transcendentals=0
        ),
    )


def read_codes(code_ref):
    lights, members = code_ref.shape
    return [[code_ref[g, j] for j in range(members)] for g in range(lights)]


def columns(ref, half):
    return ref[:, pl.ds(pl.multiple_of(half * BLOCK, BLOCK), BLOCK)]


def template_kernel(code_ref, own_ref, near_ref, far_ref, out_ref):
    lights, members = code_ref.shape
    codes = read_codes(code_ref)
    for g in range(lights):
        for j in range(members):
            code = codes[g][j]
            for place, ref in enumerate((own_ref, near_ref, far_ref)):

                @pl.when(code // 2 == place)
                def _():
                    out_ref[g, j * BLOCK : (j + 1) * BLOCK, :] = columns(ref, code % 2).T


def newton_schulz(now_ref, next_ref, gram_ref):
    lights, width, _ = now_ref.shape
    head = width - BLOCK
    over = (((1,), (1,)), ((), ()))
    for g in range(lights):
        top = now_ref[g, :head]
        corner = lax.dot_general(top, top, over, preferred_element_type=jnp.float32)
        gram_ref[g, :head, :head] = corner.astype(jnp.bfloat16)
        low = lax.dot_general(now_ref[g, head:], now_ref[g], over, preferred_element_type=jnp.float32)
        low = low.astype(jnp.bfloat16)
        gram_ref[g, head:, :] = low
        gram_ref[g, :head, head:] = low[:, :head].T
    for g in range(lights):
        now = now_ref[g]
        product = jnp.dot(gram_ref[g, :, :head], now[:head], preferred_element_type=jnp.float32)
        product += jnp.dot(gram_ref[g, :, head:], now[head:], preferred_element_type=jnp.float32)
        next_ref[g] = (1.5 * now.astype(jnp.float32) - 0.5 * product).astype(jnp.bfloat16)


def polar_kernel(subject, code_ref, tmpl_ref, own_ref, near_ref, far_ref, map_ref, cols_ref, odd_ref, gram_ref):
    lights, members = code_ref.shape
    width = members * BLOCK
    frames = own_ref.shape[0]
    codes = read_codes(code_ref)
    for g in range(lights):
        for i in range(members):
            code = codes[g][i]
            lo = g * width + i * BLOCK
            for place, ref in enumerate((own_ref, near_ref.at[subject], far_ref)):

                @pl.when(code // 2 == place)
                def _():
                    cols_ref[:, lo : lo + BLOCK] = columns(ref, code % 2)

    first_ref = map_ref if NS_STEPS % 2 == 0 else odd_ref
    row = lax.broadcasted_iota(jnp.int32, (width, width), 0)
    col = lax.broadcasted_iota(jnp.int32, (width, width), 1)
    ridge = jnp.where(row == col, RIDGE_SHIFT, 0.0)
    for g in range(lights):
        cross = jnp.dot(
            tmpl_ref[g], cols_ref[:, g * width : (g + 1) * width], preferred_element_type=jnp.float32
        )
        cross = cross * (1.0 / frames) + ridge
        squares = jnp.sum(cross * cross, keepdims=True)
        first_ref[g] = (cross * (1.0 / jnp.sqrt(squares + NORM_EPSILON))).astype(jnp.bfloat16)

    turns = (first_ref, odd_ref if first_ref is map_ref else map_ref)
    for step in range(NS_STEPS):
        newton_schulz(turns[step % 2], turns[1 - step % 2], gram_ref)


def map_kernel(subj_count, places, splits, code_ref, *refs):
    cols_refs = refs[:subj_count]
    map_refs = refs[subj_count : 2 * subj_count]
    weight_ref = refs[-1]
    out_refs = refs[2 * subj_count : -1]
    lights, members = code_ref.shape
    width = members * BLOCK
    codes = read_codes(code_ref)
    counts = []
    for p, place in enumerate(places):
        total = jnp.int32(0)
        for g in range(lights):
            pick = jnp.int32(0)
            found = codes[g][0] == place
            for j in range(1, members):
                hit = codes[g][j] == place
                pick = jnp.where(hit, j, pick)
                found = jnp.logical_or(found, hit)
            total = total + found.astype(jnp.int32)
            rows = pl.ds(pl.multiple_of(pick * BLOCK, BLOCK), BLOCK)
            for s in range(subj_count):
                lo = (s * lights + g) * width
                piece = map_refs[s][g, rows, :]
                weight_ref[p * BLOCK : (p + 1) * BLOCK, lo : lo + width] = jnp.where(
                    found, piece, jnp.zeros_like(piece)
                )
        counts.append(total)
    depth = lights * width
    group = len(places) // len(splits)
    step_cols = group * BLOCK
    chunk = 256
    at = 0
    for n, pieces in enumerate(splits):
        first = n * step_cols
        weights = [
            weight_ref[first : first + step_cols, s * depth : (s + 1) * depth] for s in range(subj_count)
        ]
        for b in range(group):
            tally = jnp.full((COUNT_ROWS, BLOCK), counts[n * group + b], jnp.int32)
            out_refs[at][pieces[0] :, b * BLOCK : (b + 1) * BLOCK] = tally.astype(jnp.float32).astype(
                out_refs[at].dtype
            )
        above = 0
        for rows in pieces:
            for lo in range(0, rows, chunk):
                total = None
                for s in range(subj_count):
                    term = lax.dot_general(
                        cols_refs[s][above + lo : above + lo + chunk, :],
                        weights[s],
                        (((1,), (1,)), ((), ())),
                        preferred_element_type=jnp.float32,
                    )
                    total = term if total is None else total + term
                out_refs[at][lo : lo + chunk, :] = total.astype(out_refs[at].dtype)
            above += rows
            at += 1


def finish_kernel(subjects, *refs):
    *pairs, cover_ref, out_ref, tile_ref, sems = refs
    rows = pairs[0].shape[0]
    scale = 1.0 / (cover_ref[...] * subjects)
    copies = []
    for h in range(len(pairs) // 2):
        total = pairs[2 * h][...].astype(jnp.float32) + pairs[2 * h + 1][...].astype(jnp.float32)
        here = pl.ds(h * rows, rows)
        tile_ref[here, :] = total * scale
        copies.append(pltpu.make_async_copy(tile_ref.at[here], out_ref.at[here], sems.at[h]))
        copies[-1].start()
    for copy in copies:
        copy.wait()


def finished(pairs, cover, subjects):
    rows, cols = pairs[0][0].shape
    count = len(pairs)
    return pl.pallas_call(
        functools.partial(finish_kernel, subjects),
        out_shape=jax.ShapeDtypeStruct((rows * count, cols), jnp.float32),
        in_specs=[vmem()] * (2 * count + 1),
        out_specs=pl.BlockSpec(memory_space=pl.ANY),
        scratch_shapes=[pltpu.VMEM((rows * count, cols), jnp.float32), pltpu.SemaphoreType.DMA((count,))],
        compiler_params=pltpu.CompilerParams(vmem_limit_bytes=LIMIT * MIB),
        name="finish",
    )(*[value for pair in pairs for value in pair], cover)


def body(series, template, sl_blocks):
    subj_count, frames, width_dev = series.shape
    lights, members = sl_blocks.shape
    blk_dev = width_dev // BLOCK
    width = members * BLOCK
    count = lax.axis_size("cortex")
    position = lax.axis_index("cortex")
    odd = position % 2
    far_real = jnp.logical_and(position + 2 * odd - 1 >= 0, position + 2 * odd - 1 < count)

    window = sl_blocks - (position - 1) * blk_dev
    side = window // blk_dev
    place = jnp.where(side == 1, 0, jnp.where((side == 2) == (odd == 1), 2, 1))
    code = (place * blk_dev + window % blk_dev).astype(jnp.int32)

    code, template, series = lax.optimization_barrier((code, template, series))

    tmpl_far = swap_far(template)
    tmpl_near = swap_near(template)
    parts = [series[s] for s in range(subj_count)]
    far = []
    for part in parts:
        far.append(swap_far(part))
    near = swap_near(series)

    tmpl_rows = call(
        template_kernel,
        jax.ShapeDtypeStruct((lights, width, frames), jnp.bfloat16),
        [vmem()] * 4,
        flops=10**9,
        limit=LIMIT,
    )(code, template, tmpl_near, tmpl_far)

    maps, cols = [], []
    for s in range(subj_count):
        polar, gathered = call(
            functools.partial(polar_kernel, s),
            (
                jax.ShapeDtypeStruct((lights, width, width), jnp.bfloat16),
                jax.ShapeDtypeStruct((frames, lights * width), jnp.bfloat16),
            ),
            [vmem()] * 5,
            flops=8 * 10**9,
            limit=LIMIT,
            scratch=[pltpu.VMEM((lights, width, width), jnp.bfloat16)] * 2,
        )(code, tmpl_rows, parts[s], near, far[s])
        maps.append(polar)
        cols.append(gathered)

    def mapped(places, splits, types):
        shapes = [
            jax.ShapeDtypeStruct((rows + (COUNT_ROWS if n == 0 else 0), width_dev), kind)
            for pieces, kind in zip(splits, types)
            for n, rows in enumerate(pieces)
        ]
        return call(
            functools.partial(map_kernel, subj_count, places, splits),
            shapes,
            [vmem()] * (1 + 2 * subj_count),
            flops=len(places) * 4 * 10**8,
            limit=LIMIT,
            scratch=[pltpu.VMEM((len(places) * BLOCK, subj_count * lights * width), jnp.bfloat16)],
        )(code, *cols, *maps)

    blocks = list(range(blk_dev))
    (to_far,) = mapped([2 * blk_dev + b for b in blocks], ((frames,),), (jnp.bfloat16,))
    from_far = swap_far(to_far)
    code, _ = lax.optimization_barrier((code, to_far))
    to_near, *own = mapped(
        [blk_dev + b for b in blocks] + blocks, ((frames,), (frames // PIECES,) * PIECES), (jnp.bfloat16, jnp.float32)
    )
    from_near = swap_near(to_near)
    keep = far_real.astype(jnp.float32)

    def joined(mine, lo, hi):
        return mine + from_near[lo:hi].astype(jnp.float32) + keep * from_far[lo:hi].astype(jnp.float32)

    rows = frames // PIECES
    per_vertex = joined(own[0][rows : rows + 1], frames, frames + 1)
    halves = [joined(own[h][:rows], h * rows, (h + 1) * rows) for h in range(PIECES)]
    subj_size = lax.axis_size("subj")
    distances = []
    while 2 ** len(distances) < subj_size:
        distances.append(2 ** len(distances))
    pairs = []
    for step in range(len(distances)):
        pairs = []
        for h in range(PIECES):
            sent = halves[h].astype(jnp.bfloat16)
            got = swap_subj(sent, distances[(step + h) % len(distances)])
            halves[h] = sent.astype(jnp.float32) + got.astype(jnp.float32)
            pairs.append((sent, got))
    if not pairs:
        return jnp.concatenate(halves, axis=0) / per_vertex / (subj_count * subj_size)
    return finished(pairs, per_vertex, subj_count * subj_size)


def solution(mesh):
    def step(series, template, sl_blocks):
        in_specs = (P("subj", None, "cortex"), P(None, "cortex"), P("cortex", None))
        out_specs = P(None, "cortex")
        placed = jax.shard_map(body, mesh=mesh, in_specs=in_specs, out_specs=out_specs, check_vma=False)
        return placed(series, template, sl_blocks)

    return step
```

```python
import functools

import jax
import jax.numpy as jnp
from jax import lax
from jax.experimental import pallas as pl
from jax.experimental.pallas import tpu as pltpu
from jax.sharding import PartitionSpec as P


BLOCK = 128
NS_STEPS = 8
RIDGE_SHIFT = 0.1
NORM_EPSILON = 1e-06
COUNT_ROWS = 16
MIB = 1 << 20
LIMIT = 24
PIECES = 4


def swap_near(value):
    count = lax.axis_size("cortex")
    return lax.ppermute(value, "cortex", [(i, i ^ 1) for i in range(count)])


def swap_far(value):
    count = lax.axis_size("cortex")
    route = [(0, 0), (count - 1, count - 1)]
    for i in range(1, count - 1, 2):
        route += [(i, i + 1), (i + 1, i)]
    return lax.ppermute(value, "cortex", route)


def swap_subj(value, distance):
    count = lax.axis_size("subj")
    return lax.ppermute(value, "subj", [(i, i ^ distance) for i in range(count)])


def vmem():
    return pl.BlockSpec(memory_space=pltpu.VMEM)


def call(kernel, out_shape, in_specs, flops, limit, scratch=()):
    outs = jax.tree.leaves(out_shape)
    return pl.pallas_call(
        kernel,
        out_shape=out_shape,
        in_specs=in_specs,
        out_specs=jax.tree.map(lambda _: vmem(), out_shape),
        scratch_shapes=list(scratch),
        compiler_params=pltpu.CompilerParams(vmem_limit_bytes=limit * MIB),
        cost_estimate=pl.CostEstimate(
            flops=flops, bytes_accessed=sum(o.size * o.dtype.itemsize for o in outs), transcendentals=0
        ),
    )


def read_codes(blocks_ref, blk_dev):
    position = lax.axis_index("cortex")
    odd = position % 2
    codes = []
    for g in range(blocks_ref.shape[0]):
        codes.append([])
        for j in range(blocks_ref.shape[1]):
            window = blocks_ref[g, j] - (position - 1) * blk_dev
            side = window // blk_dev
            place = jnp.where(side == 1, 0, jnp.where(side == 2 * odd, 2, 1))
            codes[g].append(place * blk_dev + window % blk_dev)
    return codes


def columns(ref, half):
    return ref[:, pl.ds(pl.multiple_of(half * BLOCK, BLOCK), BLOCK)]


def template_kernel(blocks_ref, own_ref, near_ref, far_ref, out_ref):
    lights, members = blocks_ref.shape
    blk_dev = own_ref.shape[1] // BLOCK
    codes = read_codes(blocks_ref, blk_dev)
    for g in range(lights):
        for j in range(members):
            code = codes[g][j]
            for place, ref in enumerate((own_ref, near_ref, far_ref)):

                @pl.when(code // blk_dev == place)
                def _():
                    out_ref[g, j * BLOCK : (j + 1) * BLOCK, :] = columns(ref, code % blk_dev).T


def newton_schulz(now_ref, next_ref, gram_ref):
    lights, width, _ = now_ref.shape
    head = width - BLOCK
    over = (((1,), (1,)), ((), ()))
    for g in range(lights):
        top = now_ref[g, :head]
        corner = lax.dot_general(top, top, over, preferred_element_type=jnp.float32)
        gram_ref[g, :head, :head] = corner.astype(jnp.bfloat16)
        low = lax.dot_general(now_ref[g, head:], now_ref[g], over, preferred_element_type=jnp.float32)
        low = low.astype(jnp.bfloat16)
        gram_ref[g, head:, :] = low
        gram_ref[g, :head, head:] = low[:, :head].T
    for g in range(lights):
        now = now_ref[g]
        product = jnp.dot(gram_ref[g, :, :head], now[:head], preferred_element_type=jnp.float32)
        product += jnp.dot(gram_ref[g, :, head:], now[head:], preferred_element_type=jnp.float32)
        next_ref[g] = (1.5 * now.astype(jnp.float32) - 0.5 * product).astype(jnp.bfloat16)


def polar_kernel(subject, blocks_ref, tmpl_ref, own_ref, near_ref, far_ref, map_ref, cols_ref, odd_ref, gram_ref):
    lights, members = blocks_ref.shape
    width = members * BLOCK
    frames = own_ref.shape[0]
    blk_dev = own_ref.shape[1] // BLOCK
    codes = read_codes(blocks_ref, blk_dev)
    for g in range(lights):
        for i in range(members):
            code = codes[g][i]
            lo = g * width + i * BLOCK
            for place, ref in enumerate((own_ref, near_ref.at[subject], far_ref)):

                @pl.when(code // blk_dev == place)
                def _():
                    cols_ref[:, lo : lo + BLOCK] = columns(ref, code % blk_dev)

    first_ref = map_ref if NS_STEPS % 2 == 0 else odd_ref
    row = lax.broadcasted_iota(jnp.int32, (width, width), 0)
    col = lax.broadcasted_iota(jnp.int32, (width, width), 1)
    ridge = jnp.where(row == col, RIDGE_SHIFT, 0.0)
    for g in range(lights):
        cross = jnp.dot(
            tmpl_ref[g], cols_ref[:, g * width : (g + 1) * width], preferred_element_type=jnp.float32
        )
        cross = cross * (1.0 / frames) + ridge
        squares = jnp.sum(cross * cross, keepdims=True)
        first_ref[g] = (cross * (1.0 / jnp.sqrt(squares + NORM_EPSILON))).astype(jnp.bfloat16)

    turns = (first_ref, odd_ref if first_ref is map_ref else map_ref)
    for step in range(NS_STEPS):
        newton_schulz(turns[step % 2], turns[1 - step % 2], gram_ref)


def map_kernel(subj_count, blk_dev, places, splits, blocks_ref, *refs):
    cols_refs = refs[:subj_count]
    map_refs = refs[subj_count : 2 * subj_count]
    weight_ref = refs[-1]
    out_refs = refs[2 * subj_count : -1]
    lights, members = blocks_ref.shape
    width = members * BLOCK
    codes = read_codes(blocks_ref, blk_dev)
    counts = []
    for p, place in enumerate(places):
        total = jnp.int32(0)
        for g in range(lights):
            pick = jnp.int32(0)
            found = codes[g][0] == place
            for j in range(1, members):
                hit = codes[g][j] == place
                pick = jnp.where(hit, j, pick)
                found = jnp.logical_or(found, hit)
            total = total + found.astype(jnp.int32)
            rows = pl.ds(pl.multiple_of(pick * BLOCK, BLOCK), BLOCK)
            for s in range(subj_count):
                lo = (s * lights + g) * width
                piece = map_refs[s][g, rows, :]
                weight_ref[p * BLOCK : (p + 1) * BLOCK, lo : lo + width] = jnp.where(
                    found, piece, jnp.zeros_like(piece)
                )
        counts.append(total)
    depth = lights * width
    group = len(places) // len(splits)
    step_cols = group * BLOCK
    chunk = 256
    at = 0
    for n, pieces in enumerate(splits):
        first = n * step_cols
        weights = [
            weight_ref[first : first + step_cols, s * depth : (s + 1) * depth] for s in range(subj_count)
        ]
        for b in range(group):
            tally = jnp.full((COUNT_ROWS, BLOCK), counts[n * group + b], jnp.int32)
            out_refs[at][pieces[0] :, b * BLOCK : (b + 1) * BLOCK] = tally.astype(jnp.float32).astype(
                out_refs[at].dtype
            )
        above = 0
        for rows in pieces:
            for lo in range(0, rows, chunk):
                total = None
                for s in range(subj_count):
                    term = lax.dot_general(
                        cols_refs[s][above + lo : above + lo + chunk, :],
                        weights[s],
                        (((1,), (1,)), ((), ())),
                        preferred_element_type=jnp.float32,
                    )
                    total = term if total is None else total + term
                out_refs[at][lo : lo + chunk, :] = total.astype(out_refs[at].dtype)
            above += rows
            at += 1


def finish_kernel(subjects, count, above, *refs):
    pairs, cover_ref = refs[: 2 * count], refs[2 * count]
    out_ref, tile_ref, sems = refs[-3:]
    rows = pairs[0].shape[0]
    scale = 1.0 / (cover_ref[...] * subjects)
    copies = []
    for h in range(count):
        total = pairs[2 * h][...].astype(jnp.float32) + pairs[2 * h + 1][...].astype(jnp.float32)
        here = pl.ds(h * rows, rows)
        tile_ref[here, :] = total * scale
        there = pl.ds((above + h) * rows, rows)
        copies.append(pltpu.make_async_copy(tile_ref.at[here], out_ref.at[there], sems.at[h]))
        copies[-1].start()
    for copy in copies:
        copy.wait()


def finished(result, frames, above, pairs, cover, subjects):
    rows, cols = pairs[0][0].shape
    count = len(pairs)
    placed = [] if result is None else [result]
    return pl.pallas_call(
        functools.partial(finish_kernel, subjects, count, above),
        out_shape=jax.ShapeDtypeStruct((frames, cols), jnp.float32),
        in_specs=[vmem()] * (2 * count + 1) + [pl.BlockSpec(memory_space=pl.ANY)] * len(placed),
        out_specs=pl.BlockSpec(memory_space=pl.ANY),
        scratch_shapes=[pltpu.VMEM((rows * count, cols), jnp.float32), pltpu.SemaphoreType.DMA((count,))],
        input_output_aliases={2 * count + 1: 0} if placed else {},
        compiler_params=pltpu.CompilerParams(vmem_limit_bytes=LIMIT * MIB),
        name="finish",
    )(*[value for pair in pairs for value in pair], cover, *placed)


def body(series, template, sl_blocks):
    subj_count, frames, width_dev = series.shape
    lights, members = sl_blocks.shape
    blk_dev = width_dev // BLOCK
    width = members * BLOCK
    count = lax.axis_size("cortex")
    position = lax.axis_index("cortex")
    odd = position % 2
    far_real = jnp.logical_and(position + 2 * odd - 1 >= 0, position + 2 * odd - 1 < count)

    tmpl_far = swap_far(template)
    tmpl_near = swap_near(template)
    parts = [series[s] for s in range(subj_count)]
    far = []
    for part in parts:
        far.append(swap_far(part))
    near = swap_near(series)

    tmpl_rows = call(
        template_kernel,
        jax.ShapeDtypeStruct((lights, width, frames), jnp.bfloat16),
        [vmem()] * 4,
        flops=10**9,
        limit=LIMIT,
    )(sl_blocks, template, tmpl_near, tmpl_far)

    maps, cols = [], []
    for s in range(subj_count):
        polar, gathered = call(
            functools.partial(polar_kernel, s),
            (
                jax.ShapeDtypeStruct((lights, width, width), jnp.bfloat16),
                jax.ShapeDtypeStruct((frames, lights * width), jnp.bfloat16),
            ),
            [vmem()] * 5,
            flops=8 * 10**9,
            limit=LIMIT,
            scratch=[pltpu.VMEM((lights, width, width), jnp.bfloat16)] * 2,
        )(sl_blocks, tmpl_rows, parts[s], near, far[s])
        maps.append(polar)
        cols.append(gathered)

    def mapped(lists, places, splits, types):
        shapes = [
            jax.ShapeDtypeStruct((rows + (COUNT_ROWS if n == 0 else 0), width_dev), kind)
            for pieces, kind in zip(splits, types)
            for n, rows in enumerate(pieces)
        ]
        return call(
            functools.partial(map_kernel, subj_count, blk_dev, places, splits),
            shapes,
            [vmem()] * (1 + 2 * subj_count),
            flops=len(places) * 4 * 10**8,
            limit=LIMIT,
            scratch=[pltpu.VMEM((len(places) * BLOCK, subj_count * lights * width), jnp.bfloat16)],
        )(lists, *cols, *maps)

    blocks = list(range(blk_dev))
    (to_far,) = mapped(sl_blocks, [2 * blk_dev + b for b in blocks], ((frames,),), (jnp.bfloat16,))
    from_far = swap_far(to_far)
    lists, _ = lax.optimization_barrier((sl_blocks, to_far))
    to_near, *own = mapped(
        lists, [blk_dev + b for b in blocks] + blocks, ((frames,), (frames // PIECES,) * PIECES), (jnp.bfloat16, jnp.float32)
    )
    from_near = swap_near(to_near)
    keep = far_real.astype(jnp.float32)

    def joined(mine, lo, hi):
        return mine + from_near[lo:hi].astype(jnp.float32) + keep * from_far[lo:hi].astype(jnp.float32)

    rows = frames // PIECES
    per_vertex = joined(own[0][rows : rows + 1], frames, frames + 1)
    halves = [joined(own[h][:rows], h * rows, (h + 1) * rows) for h in range(PIECES)]
    subj_size = lax.axis_size("subj")
    distances = []
    while 2 ** len(distances) < subj_size:
        distances.append(2 ** len(distances))
    pairs = []
    for step in range(len(distances)):
        pairs = []
        for h in range(PIECES):
            sent = halves[h].astype(jnp.bfloat16)
            got = swap_subj(sent, distances[(step + h) % len(distances)])
            halves[h] = sent.astype(jnp.float32) + got.astype(jnp.float32)
            pairs.append((sent, got))
    if not pairs:
        return jnp.concatenate(halves, axis=0) / per_vertex / (subj_count * subj_size)
    subjects = subj_count * subj_size
    result = finished(None, frames, 0, pairs[:-1], per_vertex, subjects)
    return finished(result, frames, PIECES - 1, pairs[-1:], per_vertex, subjects)


def solution(mesh):
    def step(series, template, sl_blocks):
        in_specs = (P("subj", None, "cortex"), P(None, "cortex"), P("cortex", None))
        out_specs = P(None, "cortex")
        placed = jax.shard_map(body, mesh=mesh, in_specs=in_specs, out_specs=out_specs, check_vma=False)
        return placed(series, template, sl_blocks)

    return step
```

```python
import functools

import jax
import jax.numpy as jnp
from jax import lax
from jax.experimental import pallas as pl
from jax.experimental.pallas import tpu as pltpu
from jax.sharding import PartitionSpec as P


BLOCK = 128
NS_STEPS = 8
RIDGE_SHIFT = 0.1
NORM_EPSILON = 1e-06
COUNT_ROWS = 16
MIB = 1 << 20
LIMIT = 24
PIECES = 4


def swap_near(value):
    count = lax.axis_size("cortex")
    return lax.ppermute(value, "cortex", [(i, i ^ 1) for i in range(count)])


def swap_far(value):
    count = lax.axis_size("cortex")
    route = [(0, 0), (count - 1, count - 1)]
    for i in range(1, count - 1, 2):
        route += [(i, i + 1), (i + 1, i)]
    return lax.ppermute(value, "cortex", route)


def swap_subj(value, distance):
    count = lax.axis_size("subj")
    return lax.ppermute(value, "subj", [(i, i ^ distance) for i in range(count)])


def vmem():
    return pl.BlockSpec(memory_space=pltpu.VMEM)


def call(kernel, out_shape, in_specs, flops, limit, scratch=()):
    outs = jax.tree.leaves(out_shape)
    return pl.pallas_call(
        kernel,
        out_shape=out_shape,
        in_specs=in_specs,
        out_specs=jax.tree.map(lambda _: vmem(), out_shape),
        scratch_shapes=list(scratch),
        compiler_params=pltpu.CompilerParams(vmem_limit_bytes=limit * MIB),
        cost_estimate=pl.CostEstimate(
            flops=flops, bytes_accessed=sum(o.size * o.dtype.itemsize for o in outs), transcendentals=0
        ),
    )


def read_codes(blocks_ref, blk_dev):
    position = lax.axis_index("cortex")
    odd = position % 2
    codes = []
    for g in range(blocks_ref.shape[0]):
        codes.append([])
        for j in range(blocks_ref.shape[1]):
            window = blocks_ref[g, j] - (position - 1) * blk_dev
            side = window // blk_dev
            place = jnp.where(side == 1, 0, jnp.where(side == 2 * odd, 2, 1))
            codes[g].append(place * blk_dev + window % blk_dev)
    return codes


def columns(ref, half):
    return ref[:, pl.ds(pl.multiple_of(half * BLOCK, BLOCK), BLOCK)]


def template_kernel(blocks_ref, own_ref, near_ref, far_ref, out_ref):
    lights, members = blocks_ref.shape
    blk_dev = own_ref.shape[1] // BLOCK
    codes = read_codes(blocks_ref, blk_dev)
    for g in range(lights):
        for j in range(members):
            code = codes[g][j]
            for place, ref in enumerate((own_ref, near_ref, far_ref)):

                @pl.when(code // blk_dev == place)
                def _():
                    out_ref[g, j * BLOCK : (j + 1) * BLOCK, :] = columns(ref, code % blk_dev).T


def newton_schulz(now_ref, next_ref, gram_ref):
    lights, width, _ = now_ref.shape
    head = width - BLOCK
    over = (((1,), (1,)), ((), ()))
    for g in range(lights):
        top = now_ref[g, :head]
        corner = lax.dot_general(top, top, over, preferred_element_type=jnp.float32)
        gram_ref[g, :head, :head] = corner.astype(jnp.bfloat16)
        low = lax.dot_general(now_ref[g, head:], now_ref[g], over, preferred_element_type=jnp.float32)
        low = low.astype(jnp.bfloat16)
        gram_ref[g, head:, :] = low
        gram_ref[g, :head, head:] = low[:, :head].T
    for g in range(lights):
        now = now_ref[g]
        product = jnp.dot(gram_ref[g, :, :head], now[:head], preferred_element_type=jnp.float32)
        product += jnp.dot(gram_ref[g, :, head:], now[head:], preferred_element_type=jnp.float32)
        next_ref[g] = (1.5 * now.astype(jnp.float32) - 0.5 * product).astype(jnp.bfloat16)


def polar_kernel(subject, blocks_ref, tmpl_ref, own_ref, near_ref, far_ref, map_ref, cols_ref, odd_ref, gram_ref):
    lights, members = blocks_ref.shape
    width = members * BLOCK
    frames = own_ref.shape[0]
    blk_dev = own_ref.shape[1] // BLOCK
    codes = read_codes(blocks_ref, blk_dev)
    for g in range(lights):
        for i in range(members):
            code = codes[g][i]
            lo = g * width + i * BLOCK
            for place, ref in enumerate((own_ref, near_ref.at[subject], far_ref)):

                @pl.when(code // blk_dev == place)
                def _():
                    cols_ref[:, lo : lo + BLOCK] = columns(ref, code % blk_dev)

    first_ref = map_ref if NS_STEPS % 2 == 0 else odd_ref
    row = lax.broadcasted_iota(jnp.int32, (width, width), 0)
    col = lax.broadcasted_iota(jnp.int32, (width, width), 1)
    ridge = jnp.where(row == col, RIDGE_SHIFT, 0.0)
    for g in range(lights):
        cross = jnp.dot(
            tmpl_ref[g], cols_ref[:, g * width : (g + 1) * width], preferred_element_type=jnp.float32
        )
        cross = cross * (1.0 / frames) + ridge
        squares = jnp.sum(cross * cross, keepdims=True)
        first_ref[g] = (cross * (1.0 / jnp.sqrt(squares + NORM_EPSILON))).astype(jnp.bfloat16)

    turns = (first_ref, odd_ref if first_ref is map_ref else map_ref)
    for step in range(NS_STEPS):
        newton_schulz(turns[step % 2], turns[1 - step % 2], gram_ref)


def map_kernel(subj_count, blk_dev, places, splits, blocks_ref, *refs):
    cols_refs = refs[:subj_count]
    map_refs = refs[subj_count : 2 * subj_count]
    weight_ref = refs[-1]
    out_refs = refs[2 * subj_count : -1]
    lights, members = blocks_ref.shape
    width = members * BLOCK
    codes = read_codes(blocks_ref, blk_dev)
    counts = []
    for p, place in enumerate(places):
        total = jnp.int32(0)
        for g in range(lights):
            pick = jnp.int32(0)
            found = codes[g][0] == place
            for j in range(1, members):
                hit = codes[g][j] == place
                pick = jnp.where(hit, j, pick)
                found = jnp.logical_or(found, hit)
            total = total + found.astype(jnp.int32)
            rows = pl.ds(pl.multiple_of(pick * BLOCK, BLOCK), BLOCK)
            for s in range(subj_count):
                lo = (s * lights + g) * width
                piece = map_refs[s][g, rows, :]
                weight_ref[p * BLOCK : (p + 1) * BLOCK, lo : lo + width] = jnp.where(
                    found, piece, jnp.zeros_like(piece)
                )
        counts.append(total)
    depth = lights * width
    group = len(places) // len(splits)
    step_cols = group * BLOCK
    chunk = 256
    at = 0
    for n, pieces in enumerate(splits):
        first = n * step_cols
        weights = [
            weight_ref[first : first + step_cols, s * depth : (s + 1) * depth] for s in range(subj_count)
        ]
        for b in range(group):
            tally = jnp.full((COUNT_ROWS, BLOCK), counts[n * group + b], jnp.int32)
            out_refs[at][pieces[0] :, b * BLOCK : (b + 1) * BLOCK] = tally.astype(jnp.float32).astype(
                out_refs[at].dtype
            )
        above = 0
        for rows in pieces:
            for lo in range(0, rows, chunk):
                total = None
                for s in range(subj_count):
                    term = lax.dot_general(
                        cols_refs[s][above + lo : above + lo + chunk, :],
                        weights[s],
                        (((1,), (1,)), ((), ())),
                        preferred_element_type=jnp.float32,
                    )
                    total = term if total is None else total + term
                out_refs[at][lo : lo + chunk, :] = total.astype(out_refs[at].dtype)
            above += rows
            at += 1


def finish_kernel(subjects, count, above, *refs):
    pairs, cover_ref = refs[: 2 * count], refs[2 * count]
    out_ref, tile_ref, sems = refs[-3:]
    rows = pairs[0].shape[0]
    scale = 1.0 / (cover_ref[...] * subjects)
    copies = []
    for h in range(count):
        total = pairs[2 * h][...].astype(jnp.float32) + pairs[2 * h + 1][...].astype(jnp.float32)
        here = pl.ds(h * rows, rows)
        tile_ref[here, :] = total * scale
        there = pl.ds((above + h) * rows, rows)
        copies.append(pltpu.make_async_copy(tile_ref.at[here], out_ref.at[there], sems.at[h]))
        copies[-1].start()
    for copy in copies:
        copy.wait()


def finished(result, frames, above, pairs, cover, subjects):
    rows, cols = pairs[0][0].shape
    count = len(pairs)
    placed = [] if result is None else [result]
    return pl.pallas_call(
        functools.partial(finish_kernel, subjects, count, above),
        out_shape=jax.ShapeDtypeStruct((frames, cols), jnp.float32),
        in_specs=[vmem()] * (2 * count + 1) + [pl.BlockSpec(memory_space=pl.ANY)] * len(placed),
        out_specs=pl.BlockSpec(memory_space=pl.ANY),
        scratch_shapes=[pltpu.VMEM((rows * count, cols), jnp.float32), pltpu.SemaphoreType.DMA((count,))],
        input_output_aliases={2 * count + 1: 0} if placed else {},
        compiler_params=pltpu.CompilerParams(vmem_limit_bytes=LIMIT * MIB),
        name="finish",
    )(*[value for pair in pairs for value in pair], cover, *placed)


def last_kernel(subj_count, blk_dev, places, splits, blocks_ref, tmpl_ref, own_ref, near_ref, far_ref, *refs):
    before = subj_count - 1
    cols_refs, map_refs = refs[:before], refs[before : 2 * before]
    map_ref, cols_ref, *tile_refs = refs[2 * before : -3]
    odd_ref, gram_ref, weight_ref = refs[-3:]
    polar_kernel(before, blocks_ref, tmpl_ref, own_ref, near_ref, far_ref, map_ref, cols_ref, odd_ref, gram_ref)
    map_kernel(
        subj_count, blk_dev, places, splits, blocks_ref,
        *cols_refs, cols_ref, *map_refs, map_ref, *tile_refs, weight_ref,
    )


def body(series, template, sl_blocks):
    subj_count, frames, width_dev = series.shape
    lights, members = sl_blocks.shape
    blk_dev = width_dev // BLOCK
    width = members * BLOCK
    count = lax.axis_size("cortex")
    position = lax.axis_index("cortex")
    odd = position % 2
    far_real = jnp.logical_and(position + 2 * odd - 1 >= 0, position + 2 * odd - 1 < count)

    tmpl_far = swap_far(template)
    tmpl_near = swap_near(template)
    parts = [series[s] for s in range(subj_count)]
    far = []
    for part in parts:
        far.append(swap_far(part))
    near = swap_near(series)

    tmpl_rows = call(
        template_kernel,
        jax.ShapeDtypeStruct((lights, width, frames), jnp.bfloat16),
        [vmem()] * 4,
        flops=10**9,
        limit=LIMIT,
    )(sl_blocks, template, tmpl_near, tmpl_far)

    maps, cols = [], []
    blocks = list(range(blk_dev))
    shapes = [
        jax.ShapeDtypeStruct((lights, width, width), jnp.bfloat16),
        jax.ShapeDtypeStruct((frames, lights * width), jnp.bfloat16),
    ]
    scratch = [pltpu.VMEM((lights, width, width), jnp.bfloat16)] * 2
    for s in range(subj_count):
        halo = (sl_blocks, tmpl_rows, parts[s], near, far[s])
        last = s == subj_count - 1
        if last:
            far_places = [2 * blk_dev + b for b in blocks]
            polar, gathered, to_far = call(
                functools.partial(last_kernel, subj_count, blk_dev, far_places, ((frames,),)),
                shapes + [jax.ShapeDtypeStruct((frames + COUNT_ROWS, width_dev), jnp.bfloat16)],
                [vmem()] * (5 + 2 * s),
                flops=8 * 10**9,
                limit=LIMIT,
                scratch=scratch
                + [pltpu.VMEM((blk_dev * BLOCK, subj_count * lights * width), jnp.bfloat16)],
            )(*halo, *cols, *maps)
        else:
            polar, gathered = call(
                functools.partial(polar_kernel, s), shapes, [vmem()] * 5, flops=8 * 10**9, limit=LIMIT, scratch=scratch
            )(*halo)
        maps.append(polar)
        cols.append(gathered)

    def mapped(lists, places, splits, types):
        shapes = [
            jax.ShapeDtypeStruct((rows + (COUNT_ROWS if n == 0 else 0), width_dev), kind)
            for pieces, kind in zip(splits, types)
            for n, rows in enumerate(pieces)
        ]
        return call(
            functools.partial(map_kernel, subj_count, blk_dev, places, splits),
            shapes,
            [vmem()] * (1 + 2 * subj_count),
            flops=len(places) * 4 * 10**8,
            limit=LIMIT,
            scratch=[pltpu.VMEM((len(places) * BLOCK, subj_count * lights * width), jnp.bfloat16)],
        )(lists, *cols, *maps)

    from_far = swap_far(to_far)
    lists, _ = lax.optimization_barrier((sl_blocks, to_far))
    to_near, *own = mapped(
        lists, [blk_dev + b for b in blocks] + blocks, ((frames,), (frames // PIECES,) * PIECES), (jnp.bfloat16, jnp.float32)
    )
    from_near = swap_near(to_near)
    keep = far_real.astype(jnp.float32)

    def joined(mine, lo, hi):
        return mine + from_near[lo:hi].astype(jnp.float32) + keep * from_far[lo:hi].astype(jnp.float32)

    rows = frames // PIECES
    halves = [joined(own[0][:rows], 0, rows).astype(jnp.bfloat16)]
    halves[0], from_far, from_near = lax.optimization_barrier((halves[0], from_far, from_near))
    halves += [joined(own[h][:rows], h * rows, (h + 1) * rows) for h in range(1, PIECES)]
    subj_size = lax.axis_size("subj")
    distances = []
    while 2 ** len(distances) < subj_size:
        distances.append(2 ** len(distances))
    per_vertex = joined(own[0][rows : rows + 1], frames, frames + 1)
    pairs = []
    for step in range(len(distances)):
        pairs = []
        for h in range(PIECES):
            sent = halves[h].astype(jnp.bfloat16)
            got = swap_subj(sent, distances[(step + h) % len(distances)])
            halves[h] = sent.astype(jnp.float32) + got.astype(jnp.float32)
            pairs.append((sent, got))
    if not pairs:
        return jnp.concatenate(halves, axis=0) / per_vertex / (subj_count * subj_size)
    subjects = subj_count * subj_size
    result = finished(None, frames, 0, pairs[:-1], per_vertex, subjects)
    return finished(result, frames, PIECES - 1, pairs[-1:], per_vertex, subjects)


def solution(mesh):
    def step(series, template, sl_blocks):
        in_specs = (P("subj", None, "cortex"), P(None, "cortex"), P("cortex", None))
        out_specs = P(None, "cortex")
        placed = jax.shard_map(body, mesh=mesh, in_specs=in_specs, out_specs=out_specs, check_vma=False)
        return placed(series, template, sl_blocks)

    return step
```
